32 devices in a mesh: group: 2 (over y), seq: 4 (over z), head: 4 (over x, core), pair: 1.
Axes of the slice: x: 2, y: 2, z: 4, core: 2. Of those that a mesh axis runs over, the one named last changes fastest.
Arguments:
- query_states: bfloat16 [2048, 4096], P(('group', 'seq'), ('head', 'pair')), parts along dimension 0, may hold values from -6 to 6
- key_states: bfloat16 [2048, 512], P(('group', 'seq'), 'head'), parts along dimension 0, may hold values from -6 to 6
- value_states: bfloat16 [2048, 512], P(('group', 'seq'), 'head'), parts along dimension 0, may hold values from -12 to 12
- sink_logits: float32 [64], P(('head', 'pair')), may hold values from 0 to 5
- segment_ids: int32 [2048], P('group'), parts along dimension 0, may hold values from 0 to 11, never falling along the last dimension, each value on 1 to 256 neighbouring positions
- residual: bfloat16 [2048, 1536], P(('group', 'seq', 'head', 'pair')), parts along dimension 0, may hold values from -6 to 6
- out_weight: bfloat16 [4096, 1536], P(('head', 'pair')), may hold values from -0.09375 to 0.09375
- norm_gain: float32 [1536], replicated, may hold values from 0.5 to 1.5
- expert_ids: int32 [2048, 4], P(('group', 'seq', 'head', 'pair')), parts along dimension 0, may hold values from 0 to 7, all different within a row; in each aligned block of 64 rows (0 to 63, 64 to 127, ...) at most 48 rows name the same one
- route_weights: float32 [2048, 4], P(('group', 'seq', 'head', 'pair')), parts along dimension 0, may hold values from 0.1 to 1
- gate_proj: bfloat16 [16, 1536, 768], P(('seq', 'head'), None, 'pair'), may hold values from -0.15625 to 0.15625
- up_proj: bfloat16 [16, 1536, 768], P(('seq', 'head'), None, 'pair'), may hold values from -0.15625 to 0.15625
- down_proj: bfloat16 [16, 768, 1536], P(('seq', 'head'), 'pair'), may hold values from -0.15625 to 0.15625
Outputs:
- layer_out: bfloat16 [2048, 1536], P(('group', 'seq', 'head', 'pair')), parts along dimension 0
The draws below stay inside these ranges and needn't reach their ends.
There are 2 independent parts, one for each index of `group`. The reference program is written for one: setup_inputs(seed, part) draws one part's arguments, and reference() takes and returns one part's arrays. A program takes and returns all parts, laid end to end along the dimension named above; an argument that names none is the same for every part. Nothing has to cross between parts.
Inputs may be any that keep to these rules, and one draw needn't show every extreme that they name: `segment_ids`: never falling along the sequence; each passage holds 1 to 256 tokens and one holds exactly 256. `expert_ids`: each row names 4 different experts. Among the rows of one device (aligned blocks of 64 rows) no expert is named by more than 48 rows, a bound that some block reaches.
All inputs are finite; a program needn't handle non-finite values.
Results may differ from the reference program's by a relative error of at most 0.015.
Values may be sent and summed in bfloat16 or wider, within the bound.
No kernel may reach another device: no remote copies, remote signals or barrier semaphores. Data moves between devices by JAX's collectives and lax.ppermute only.
A program may use at most 64 MiB of HBM per device.

```python
import math
import jax
import jax.numpy as jnp
import numpy as np
from jax import lax

D = 1536
FF = 1536
HEADS = 64
KV_HEADS = 8
HEAD_DIM = 64
TOP = 4
WINDOW = 128
TOK_DEV = 256
TOKENS = 1024
TOK_SHARD = 64
HEAD_BLOCK = 16
EXPERTS = 8
EXPERT_HALVES = 16
FF_HALF = 768
FF_QUARTER = 384
CAP = 48
SEGMENTS = 12


def draw_query_states(key, part):
    shape = (TOKENS, HEADS * HEAD_DIM)
    result = jnp.clip(jax.random.normal(jax.random.fold_in(key, 12), shape), -6.0, 6.0)
    return result.astype(jnp.bfloat16)


def draw_key_states(key, part):
    shape = (TOKENS, KV_HEADS * HEAD_DIM)
    result = jnp.clip(jax.random.normal(jax.random.fold_in(key, 22), shape), -6.0, 6.0)
    return result.astype(jnp.bfloat16)


def block_scale(rng, shape, split, least, top_value):
    factor_of, own = 1.0, jax.random.fold_in(rng, 6)
    for axis_at, shards_of in split:
        steps = jnp.exp(jax.random.uniform(jax.random.fold_in(own, axis_at), (shards_of,), jnp.float32, least / len(split), top_value / len(split)))
        factor_of = factor_of * jnp.repeat(steps, shape[axis_at] // shards_of).reshape([-1 if axis == axis_at else 1 for axis in range(len(shape))])
    return factor_of


def length_profile(amount, total, reach, lean):
    portions = [(1 << 20) // math.isqrt(grade ** lean) + 1 for grade in range(2, amount + 1)]
    spare, holding = total - reach - (amount - 1), [1] * (amount - 1)
    while spare > 0:
        movable = [i for i in range(amount - 1) if holding[i] < reach]
        pool, remaining = sum([portions[i] for i in movable]), spare
        for i in movable:
            addition = min(reach - holding[i], max(1, remaining * portions[i] // pool), spare)
            holding[i] = holding[i] + addition
            spare = spare - addition
    return np.array([reach] + holding)


def uneven_parts(rng, amount, total, limit, lean):
    if amount == 2:
        one = jax.random.randint(rng, (), max(1, total - limit), min(limit, total - 1) + 1)
        return jnp.stack([one, total - one])
    lengths = jnp.asarray(length_profile(amount, total, limit, lean), jnp.int32)
    twos = (amount - 1) // 2
    source_of, receiver = lengths[1:1 + 2 * twos:2], lengths[2:2 + 2 * twos:2]
    margin = jnp.minimum(source_of - 1, limit - receiver)
    moved = jax.random.randint(jax.random.fold_in(rng, 1), (twos,), 0, 1 << 20) % (margin + 1)
    lengths = lengths.at[1:1 + 2 * twos:2].set(source_of - moved).at[2:2 + 2 * twos:2].set(receiver + moved)
    return lengths[jax.random.permutation(jax.random.fold_in(rng, 2), amount)]


def shared_out(own_key, own, number, rows, amount, top, most, lean):
    order = jax.random.permutation(own_key, amount)
    packed, common = load_shares(amount, rows * top, most, lean, True), load_shares(amount, rows * top, most, lean, False)
    places = jnp.arange(amount)

    def named(lengths, turn):
        used = int((lengths > 0).sum())
        fixed = max(1, used // 4)
        moved = fixed + (places - fixed + turn * (used - fixed)) % max(1, amount - fixed)
        return jnp.zeros((amount,), jnp.int32).at[order[jnp.where(places < fixed, places, moved)]].set(jnp.asarray(lengths, jnp.int32))

    lengths = jnp.where(number % 4 == 0, named(packed, number // 4), named(common, number - number // 4 - 1))
    mixed = jax.random.permutation(jax.random.fold_in(own, 3), amount)
    giver, sink = mixed[0:amount // 2 * 2:2], mixed[1:amount // 2 * 2:2]
    margin = jnp.minimum(lengths[giver] - 1, most - lengths[sink]) // 2
    margin = jnp.where((giver == order[0]) | (sink == order[0]) | (lengths[sink] == 0), 0, jnp.maximum(margin, 0))
    moved = jax.random.randint(jax.random.fold_in(own, 4), (amount // 2,), 0, 1 << 20) % (margin + 1)
    lengths = lengths.at[giver].add(-moved).at[sink].add(moved)
    members = jnp.searchsorted(jnp.cumsum(lengths), jnp.arange(rows * top), side="right").astype(jnp.int32)
    table = members.reshape(top, rows).T
    table = table[jax.random.permutation(jax.random.fold_in(own, 1), rows)]
    turn = jax.random.randint(jax.random.fold_in(own, 2), (rows, 1), 0, top)
    return jnp.take_along_axis(table, (jnp.arange(top)[None, :] + turn) % top, axis=1)


def load_shares(number_of, total, most, skew, full):
    portions = [(1 << 20) // math.isqrt(grade ** skew) + 1 for grade in range(1, number_of + 1)]
    largest = most if full else min(most, max(-(-total // number_of), total * portions[0] // sum(portions)))
    least = 1 if total - largest >= number_of - 1 else 0
    given, spare = [largest] + [least] * (number_of - 1), total - largest - least * (number_of - 1)
    while spare > 0:
        movable = [i for i in range(1, number_of) if given[i] < largest] or [i for i in range(1, number_of) if given[i] < most]
        mass, budget = sum([portions[i] for i in movable]), spare
        for i in movable:
            extra = min(most - given[i], max(1, budget * portions[i] // mass), spare)
            given[i] = given[i] + extra
            spare = spare - extra
    return np.array(given)


def normal_values(own_key, dims, spread, most, pieces=(), kind=jnp.bfloat16):
    drawn = spread * jax.random.normal(own_key, dims, jnp.float32)
    if pieces:
        drawn = drawn * block_scale(own_key, dims, pieces, -0.22, 0.18)
    return jnp.clip(drawn, -most, most).astype(kind)


def setup_inputs(seed: int = 0, part: int = 0) -> dict:
    arg_keys = jax.random.split(jax.random.key(seed), 14)
    own_keys = jax.random.split(jax.random.fold_in(arg_keys[13], part), 14)
    query_states = draw_query_states(jax.random.fold_in(jax.random.fold_in(arg_keys[13], part), 71), part)
    key_states = draw_key_states(jax.random.fold_in(jax.random.fold_in(arg_keys[13], part), 71), part)
    value_states = normal_values(own_keys[2], (TOKENS, KV_HEADS * HEAD_DIM), 2.0, 12.0, ((0, 4), (1, 4)))
    sink_logits = jnp.clip(5.0 * jax.random.uniform(arg_keys[3], (HEADS,), jnp.float32) ** block_scale(arg_keys[3], (HEADS,), ((0, 4),), -0.2, 0.2), 0.0, 5.0)
    segment_ids = jnp.searchsorted(jnp.cumsum(uneven_parts(own_keys[4], SEGMENTS, TOKENS, TOK_DEV, 1)), jnp.arange(TOKENS), side="right").astype(jnp.int32)
    residual = normal_values(own_keys[5], (TOKENS, D), 1.0, 6.0, ((0, 16),))
    out_weight = normal_values(arg_keys[6], (HEADS * HEAD_DIM, D), (HEADS * HEAD_DIM) ** -0.5, 0.09375, ((0, 4),))
    norm_gain = jnp.clip(1.0 + 0.1 * jax.random.normal(arg_keys[7], (D,), jnp.float32), 0.5, 1.5)
    expert_ids_keys = jax.random.split(jax.random.fold_in(own_keys[8], 1), TOKENS // TOK_SHARD)
    expert_ids_turns = jax.random.permutation(jax.random.fold_in(own_keys[8], 3), TOKENS // TOK_SHARD)
    expert_ids = jax.vmap(lambda own, number: shared_out(jax.random.fold_in(own_keys[8], 2), own, number, TOK_SHARD, EXPERTS, TOP, CAP, 2))(expert_ids_keys, expert_ids_turns).reshape((TOKENS, TOP))
    route_weights = jnp.clip(jnp.exp(math.log(1.0) - 2.3025851 * jax.random.uniform(own_keys[9], (TOKENS, TOP), jnp.float32) ** block_scale(own_keys[9], (TOKENS, TOP), ((0, 16),), -0.2, 0.2)), 0.1, 1.0)
    gate_proj = normal_values(arg_keys[10], (EXPERT_HALVES, D, FF_HALF), D ** -0.5, 0.15625, ((0, 16),))
    up_proj = normal_values(arg_keys[11], (EXPERT_HALVES, D, FF_HALF), D ** -0.5, 0.15625, ((0, 16),))
    down_proj = normal_values(arg_keys[12], (EXPERT_HALVES, FF_HALF, D), FF ** -0.5, 0.15625, ((0, 16),))
    return {"query_states": query_states, "key_states": key_states, "value_states": value_states, "sink_logits": sink_logits, "segment_ids": segment_ids, "residual": residual, "out_weight": out_weight, "norm_gain": norm_gain, "expert_ids": expert_ids, "route_weights": route_weights, "gate_proj": gate_proj, "up_proj": up_proj, "down_proj": down_proj}


def round_keep(values):
    return lax.optimization_barrier(values.astype(jnp.bfloat16)).astype(jnp.float32)

def attention(query_states, key_states, value_states, sink_logits, segment_ids):
    group_size = HEADS // KV_HEADS
    block_rows = min(512, TOK_DEV)
    key_padded = jnp.concatenate([jnp.zeros((WINDOW, KV_HEADS * HEAD_DIM), jnp.bfloat16), key_states], 0)
    value_padded = jnp.concatenate([jnp.zeros((WINDOW, KV_HEADS * HEAD_DIM), jnp.bfloat16), value_states], 0)
    seg_padded = jnp.concatenate([jnp.full((WINDOW,), -1, jnp.int32), segment_ids.astype(jnp.int32)], 0)

    def attend(block_index):
        first_row = block_index * block_rows
        query_block = lax.dynamic_slice_in_dim(query_states, first_row, block_rows, 0).astype(jnp.float32)
        query_block = query_block.reshape(block_rows, HEADS, HEAD_DIM)
        key_block = lax.dynamic_slice_in_dim(key_padded, first_row, block_rows + WINDOW, 0).astype(jnp.float32)
        key_block = jnp.repeat(key_block.reshape(block_rows + WINDOW, KV_HEADS, HEAD_DIM), group_size, axis=1)
        value_block = lax.dynamic_slice_in_dim(value_padded, first_row, block_rows + WINDOW, 0).astype(jnp.float32)
        value_block = jnp.repeat(value_block.reshape(block_rows + WINDOW, KV_HEADS, HEAD_DIM), group_size, axis=1)
        query_pos = first_row + jnp.arange(block_rows, dtype=jnp.int32)
        key_pos = first_row - WINDOW + jnp.arange(block_rows + WINDOW, dtype=jnp.int32)
        query_seg = lax.dynamic_slice_in_dim(segment_ids.astype(jnp.int32), first_row, block_rows, 0)
        key_seg = lax.dynamic_slice_in_dim(seg_padded, first_row, block_rows + WINDOW, 0)
        scores = jnp.einsum('qhd,khd->hqk', query_block, key_block) * HEAD_DIM ** (-0.5)
        visible = (key_pos[None, :] <= query_pos[:, None]) & (query_pos[:, None] - key_pos[None, :] < WINDOW)
        visible = visible & (key_pos[None, :] >= 0) & (key_seg[None, :] == query_seg[:, None])
        masked = jnp.where(visible[None], scores, -1e+30)
        row_max = jnp.maximum(lax.optimization_barrier(jnp.max(masked, -1)), sink_logits[:, None])
        weights_exp = jnp.exp(masked - row_max[..., None])
        denominator = lax.optimization_barrier(jnp.sum(weights_exp, -1)) + jnp.exp(sink_logits[:, None] - row_max)
        probs = (weights_exp / denominator[..., None]).astype(jnp.bfloat16)
        attended = jnp.einsum('hqk,khd->qhd', probs.astype(jnp.float32), value_block)
        return attended.astype(jnp.bfloat16).reshape(block_rows, HEADS * HEAD_DIM)
    blocks = lax.map(attend, jnp.arange(TOKENS // block_rows, dtype=jnp.int32))
    return blocks.reshape(TOKENS, HEADS * HEAD_DIM)

def reference(query_states, key_states, value_states, sink_logits, segment_ids, residual, out_weight, norm_gain, expert_ids, route_weights, gate_proj, up_proj, down_proj):
    attended = attention(query_states, key_states, value_states, sink_logits, segment_ids)
    width_block = HEAD_BLOCK * HEAD_DIM
    hidden_state = residual.astype(jnp.float32)
    for block_index in range(HEADS // HEAD_BLOCK):
        columns = attended[:, block_index * width_block:(block_index + 1) * width_block]
        rows_w = out_weight[block_index * width_block:(block_index + 1) * width_block]
        hidden_state = hidden_state + round_keep(jnp.dot(columns, rows_w, preferred_element_type=jnp.float32))
    variance = lax.optimization_barrier(jnp.mean(hidden_state * hidden_state, -1, keepdims=True))
    normed = (hidden_state * lax.rsqrt(variance + 1e-05) * norm_gain).astype(jnp.bfloat16)
    sources = TOKENS // TOK_SHARD
    assigned = TOK_SHARD * TOP
    slot_rows = sources * CAP
    id_blocks = expert_ids.astype(jnp.int32).reshape(sources, assigned)
    onehot = (id_blocks[..., None] == jnp.arange(EXPERTS, dtype=jnp.int32)).astype(jnp.int32)
    before = jnp.cumsum(onehot, axis=1, dtype=jnp.int32) - onehot
    slot_rank = lax.optimization_barrier(jnp.sum(before * onehot, -1)).astype(jnp.int32)
    source_index = jnp.arange(sources, dtype=jnp.int32)[:, None]
    slot_index = id_blocks * slot_rows + source_index * CAP + slot_rank
    token_index = source_index * TOK_SHARD + jnp.arange(assigned, dtype=jnp.int32)[None, :] // TOP
    token_table = jnp.zeros((EXPERTS * slot_rows,), jnp.int32).at[slot_index.reshape(-1)].set(token_index.reshape(-1))
    weight_table = jnp.zeros((EXPERTS * slot_rows,), jnp.float32).at[slot_index.reshape(-1)].set(route_weights.reshape(-1))
    token_table = token_table.reshape(EXPERTS, slot_rows)
    weight_table = weight_table.reshape(EXPERTS, slot_rows)
    gate_four = gate_proj.reshape(EXPERTS, 2, D, FF_HALF)
    up_four = up_proj.reshape(EXPERTS, 2, D, FF_HALF)
    down_four = down_proj.reshape(EXPERTS, 2, FF_HALF, D)

    def one_expert(totals, inputs):
        gate_e, up_e, down_e, tokens_e, weights_e = inputs
        rows = jnp.take(normed, tokens_e, axis=0)
        expert_out = jnp.zeros((slot_rows, D), jnp.float32)
        for half_idx in range(2):
            gate_val = jnp.minimum(jnp.dot(rows, gate_e[half_idx], preferred_element_type=jnp.float32), 7.0)
            up_val = jnp.clip(jnp.dot(rows, up_e[half_idx], preferred_element_type=jnp.float32), -7.0, 7.0)
            activated = ((up_val + 1.0) * gate_val * jax.nn.sigmoid(1.702 * gate_val)).astype(jnp.bfloat16)
            for quarter_idx in range(2):
                low = quarter_idx * FF_QUARTER
                partial_value = jnp.dot(activated[:, low:low + FF_QUARTER], down_e[half_idx][low:low + FF_QUARTER], preferred_element_type=jnp.float32)
                expert_out = expert_out + round_keep(partial_value)
        totals = totals.at[tokens_e].add(weights_e[:, None] * expert_out)
        return (totals, None)
    mixture, unused = lax.scan(one_expert, jnp.zeros((TOKENS, D), jnp.float32), (gate_four, up_four, down_four, token_table, weight_table))
    return (hidden_state + mixture).astype(jnp.bfloat16)
```

```python
import functools

import jax
import jax.numpy as jnp
from jax import lax
from jax.experimental import pallas as pl
from jax.experimental.pallas import tpu as pltpu
from jax.sharding import PartitionSpec as P

HEADS = 64
KV_HEADS = 8
HEAD_DIM = 64
WINDOW = 128
LANES = 128


def passed_along(value, axis, by):
    peers = lax.axis_size(axis)
    pairs = [(i, i + by) for i in range(peers) if 0 <= i + by < peers]
    return lax.ppermute(value, axis, pairs)


def partner(value, axis, distance):
    return lax.ppermute(value, axis, [(i, i ^ 1 << distance) for i in range(lax.axis_size(axis))])


def round_keep(values):
    return lax.optimization_barrier(values.astype(jnp.bfloat16)).astype(jnp.float32)


def window_attention(
    query_block, key_block, value_block, query_pos, key_pos, query_seg, key_seg, sink_logits
):
    scores = jnp.einsum(
        "qhd,khd->hqk", query_block, key_block, preferred_element_type=jnp.float32
    ) * HEAD_DIM ** (-0.5)
    visible = (key_pos[None, :] <= query_pos[:, None]) & (
        query_pos[:, None] - key_pos[None, :] < WINDOW
    )
    visible = visible & (key_pos[None, :] >= 0) & (key_seg[None, :] == query_seg[:, None])
    masked = jnp.where(visible[None], scores, -1e30)
    row_max = jnp.maximum(jnp.max(masked, -1), sink_logits[:, None])
    weights_exp = jnp.exp(masked - row_max[..., None])
    denominator = jnp.sum(weights_exp, -1) + jnp.exp(sink_logits[:, None] - row_max)
    probs = (weights_exp / denominator[..., None]).astype(jnp.bfloat16)
    attended = jnp.einsum("hqk,khd->qhd", probs, value_block, preferred_element_type=jnp.float32)
    return attended.astype(jnp.bfloat16)


def attention(query_states, key_states, value_states, sink_logits, segment_ids):
    tok_rows = query_states.shape[0]
    local_heads = query_states.shape[1] // HEAD_DIM
    local_groups = key_states.shape[1] // HEAD_DIM
    group_size = HEADS // KV_HEADS
    tail_keys, tail_values = passed_along(
        (key_states[tok_rows - WINDOW :], value_states[tok_rows - WINDOW :]), "seq", 1
    )
    ext_keys = jnp.concatenate([tail_keys, key_states], 0).reshape(
        tok_rows + WINDOW, local_groups, HEAD_DIM
    )
    ext_values = jnp.concatenate([tail_values, value_states], 0).reshape(
        tok_rows + WINDOW, local_groups, HEAD_DIM
    )
    kv_owner = (
        lax.axis_index("pair") * local_heads + jnp.arange(local_heads, dtype=jnp.int32)
    ) // group_size
    head_select = (kv_owner[:, None] == jnp.arange(local_groups, dtype=jnp.int32)[None, :]).astype(
        jnp.bfloat16
    )
    keys_per_head = jnp.einsum(
        "kcd,hc->khd", ext_keys, head_select, preferred_element_type=jnp.float32
    ).astype(jnp.bfloat16)
    values_per_head = jnp.einsum(
        "kcd,hc->khd", ext_values, head_select, preferred_element_type=jnp.float32
    ).astype(jnp.bfloat16)
    query_heads = query_states.reshape(tok_rows, local_heads, HEAD_DIM)
    seq_start = lax.axis_index("seq") * tok_rows
    seg_padded = jnp.concatenate([jnp.full((WINDOW,), -1, jnp.int32), segment_ids], 0)
    block_rows = min(512, tok_rows)

    def attend(block_index):
        first_row = block_index * block_rows
        query_pos = seq_start + first_row + jnp.arange(block_rows, dtype=jnp.int32)
        key_pos = seq_start + first_row - WINDOW + jnp.arange(block_rows + WINDOW, dtype=jnp.int32)
        query_seg = lax.dynamic_slice_in_dim(segment_ids, seq_start + first_row, block_rows, 0)
        key_seg = lax.dynamic_slice_in_dim(
            seg_padded, seq_start + first_row, block_rows + WINDOW, 0
        )
        return window_attention(
            query_heads,
            keys_per_head,
            values_per_head,
            query_pos,
            key_pos,
            query_seg,
            key_seg,
            sink_logits,
        )

    attended = lax.map(attend, jnp.arange(tok_rows // block_rows, dtype=jnp.int32))
    return attended.reshape(tok_rows, local_heads * HEAD_DIM)


def rms_normed(hidden_state, norm_gain):
    variance = jnp.mean(hidden_state * hidden_state, -1, keepdims=True)
    return (hidden_state * lax.rsqrt(variance + 1e-05) * norm_gain).astype(jnp.bfloat16)


def exchanged_layer(
    attended,
    residual,
    out_weight,
    norm_gain,
    expert_ids,
    route_weights,
    gate_proj,
    up_proj,
    down_proj,
):
    shard_rows = residual.shape[0]
    width = residual.shape[1]
    projected = lax.psum_scatter(
        round_keep(jnp.dot(attended, out_weight, preferred_element_type=jnp.float32)).astype(
            jnp.bfloat16
        ),
        ("head", "pair"),
        scatter_dimension=0,
        tiled=True,
    ).astype(jnp.float32)
    hidden_state = residual.astype(jnp.float32) + projected
    normed = rms_normed(hidden_state, norm_gain)
    top_count = expert_ids.shape[1]
    experts = lax.axis_size("seq") * lax.axis_size("head") // 2
    capacity = min(shard_rows, max(2, 3 * shard_rows * top_count // (2 * experts)))
    flat_ids = expert_ids.reshape(-1)
    onehot = (flat_ids[:, None] == jnp.arange(experts, dtype=jnp.int32)[None, :]).astype(jnp.int32)
    before = jnp.cumsum(onehot, axis=0, dtype=jnp.int32) - onehot
    slot_rank = jnp.sum(before * onehot, -1)
    slot_index = flat_ids * capacity + slot_rank
    dispatch_mat = (
        slot_index[None, :] == jnp.arange(experts * capacity, dtype=jnp.int32)[:, None]
    ).astype(jnp.bfloat16)
    repeated = jnp.repeat(normed, top_count, axis=0)
    outgoing = jnp.dot(dispatch_mat, repeated, preferred_element_type=jnp.float32).astype(
        jnp.bfloat16
    )
    outgoing = outgoing.reshape(experts, capacity, width)
    half_idx = lax.axis_index("head") % 2
    half_width = width // 2
    split_rows = outgoing.reshape(experts, capacity, 2, half_width).transpose(0, 2, 1, 3)
    split_rows = split_rows.reshape(2 * experts, capacity, half_width)
    own_half = lax.all_to_all(split_rows, ("seq", "head"), split_axis=0, concat_axis=0, tiled=True)
    other_half = partner(own_half, "head", 0)
    arrived = jnp.where(
        half_idx == 0,
        jnp.concatenate([own_half, other_half], -1),
        jnp.concatenate([other_half, own_half], -1),
    )
    piece_rows = lax.all_gather(arrived, "pair", axis=0, tiled=True)
    flat_rows = piece_rows.reshape(-1, width)
    gate_val = jnp.minimum(
        jnp.dot(flat_rows, gate_proj[0], preferred_element_type=jnp.float32), 7.0
    )
    up_val = jnp.clip(
        jnp.dot(flat_rows, up_proj[0], preferred_element_type=jnp.float32), -7.0, 7.0
    )
    activated = ((up_val + 1.0) * gate_val * jax.nn.sigmoid(1.702 * gate_val)).astype(jnp.bfloat16)
    partial_value = round_keep(jnp.dot(activated, down_proj[0], preferred_element_type=jnp.float32))
    quarter_terms = partial_value.reshape(piece_rows.shape)
    pair_sums = lax.psum_scatter(
        quarter_terms.astype(jnp.bfloat16), "pair", scatter_dimension=0, tiled=True
    ).astype(jnp.float32)
    kept_half = lax.dynamic_slice_in_dim(pair_sums, half_idx * half_width, half_width, 2)
    given_half = lax.dynamic_slice_in_dim(pair_sums, (1 - half_idx) * half_width, half_width, 2)
    partner_half = partner(given_half.astype(jnp.bfloat16), "head", 0).astype(given_half.dtype)
    merged = kept_half + partner_half
    returned = lax.all_to_all(
        merged.astype(jnp.bfloat16), ("seq", "head"), split_axis=0, concat_axis=0, tiled=True
    ).astype(merged.dtype)
    expert_out = (
        returned.reshape(experts, 2, capacity, half_width)
        .transpose(0, 2, 1, 3)
        .reshape(experts, capacity, width)
    )
    slot_table = slot_index.reshape(shard_rows, top_count)
    columns_all = jnp.arange(experts * capacity, dtype=jnp.int32)
    combine_mat = jnp.sum(
        jnp.where(
            slot_table[:, :, None] == columns_all[None, None, :], route_weights[:, :, None], 0.0
        ),
        axis=1,
    )
    mixture = jnp.dot(
        combine_mat, expert_out.reshape(experts * capacity, width), precision=lax.Precision.HIGHEST
    )
    return (hidden_state + mixture).astype(jnp.bfloat16)


def ffn_body(experts, blocks, *refs):
    ins = refs[:blocks]
    expert_ref, gate_ref, up_ref, down_ref = refs[blocks : blocks + 4]
    outs = refs[blocks + 4 : 2 * blocks + 4]
    rows_ref, act_ref = refs[2 * blocks + 4 :]
    width, hidden = gate_ref.shape[1], gate_ref.shape[2]
    expert = expert_ref[0, 0]
    scales = []
    start = 0
    for ref in ins:
        count = ref.shape[0]
        rows_ref[start : start + count, :] = ref[:, :width]
        coded = ref[:, width:].astype(jnp.float32)
        lane = lax.broadcasted_iota(jnp.int32, coded.shape, 1)
        mine = (lane == expert) | (lane == expert + experts) | (lane == expert + 2 * experts)
        scales.append(jnp.sum(jnp.where(mine, coded, 0.0), -1, keepdims=True))
        start += count
    tile = 256
    for low in range(0, hidden, tile):
        cols = slice(low, low + tile)
        gate_val = jnp.minimum(
            jnp.dot(rows_ref[...], gate_ref[0, :, cols], preferred_element_type=jnp.float32), 7.0
        )
        up_val = jnp.clip(
            jnp.dot(rows_ref[...], up_ref[0, :, cols], preferred_element_type=jnp.float32),
            -7.0,
            7.0,
        )
        act_ref[:, cols] = ((up_val + 1.0) * gate_val * jax.nn.sigmoid(1.702 * gate_val)).astype(
            act_ref.dtype
        )
    tile = 512
    for low in range(0, width, tile):
        cols = slice(low, low + tile)
        value = jnp.dot(act_ref[...], down_ref[0, :, cols], preferred_element_type=jnp.float32)
        start = 0
        for out, scale in zip(outs, scales):
            count = out.shape[0]
            out[:, cols] = (value[start : start + count] * scale).astype(out.dtype)
            start += count


def expert_terms(blocks, expert, experts, gate_proj, up_proj, down_proj):
    width, hidden = gate_proj.shape[1], gate_proj.shape[2]
    rows = sum(block.shape[0] for block in blocks)
    whole = pl.BlockSpec(memory_space=pltpu.VMEM)
    return pl.pallas_call(
        functools.partial(ffn_body, experts, len(blocks)),
        out_shape=[jax.ShapeDtypeStruct((b.shape[0], width), jnp.bfloat16) for b in blocks],
        in_specs=[whole] * len(blocks)
        + [pl.BlockSpec(memory_space=pltpu.SMEM)]
        + [whole] * 3,
        out_specs=[whole] * len(blocks),
        scratch_shapes=[
            pltpu.VMEM((rows, width), jnp.bfloat16),
            pltpu.VMEM((rows, hidden), jnp.bfloat16),
        ],
        compiler_params=pltpu.CompilerParams(vmem_limit_bytes=24 << 20),
        cost_estimate=pl.CostEstimate(
            flops=6 * rows * width * hidden,
            bytes_accessed=6 * width * hidden + 4 * rows * width,
            transcendentals=rows * hidden,
        ),
        name="expert_terms",
    )(*blocks, expert, gate_proj, up_proj, down_proj)


def ring_layer(
    attended,
    residual,
    out_weight,
    norm_gain,
    expert_ids,
    route_weights,
    gate_proj,
    up_proj,
    down_proj,
):
    shard_rows = residual.shape[0]
    width = residual.shape[1]
    seq, head = lax.axis_size("seq"), lax.axis_size("head")
    columns = head // 2
    chips = seq * columns
    experts = chips
    core = lax.axis_index("head") % 2
    column = lax.axis_index("head") // 2

    order = [
        (col, row if col % 2 == 0 else seq - 1 - row) for col in range(columns) for row in range(seq)
    ]

    def device(place, which):
        col, row = order[place % chips]
        return row * head + col * 2 + which

    around = [(device(p, 0), device(p + 1, 0)) for p in range(chips)]
    around += [(device(p, 1), device(p - 1, 1)) for p in range(chips)]

    def ring(value):
        return lax.ppermute(value, ("seq", "head"), around)

    def swap(value):
        return partner(value, "head", 0)

    block_proj = jnp.dot(attended, out_weight, preferred_element_type=jnp.float32).astype(
        jnp.bfloat16
    )
    by_owner = block_proj.reshape(columns, 2, shard_rows, width)
    kept = lax.dynamic_index_in_dim(by_owner, core, 1, keepdims=False)
    given = lax.dynamic_index_in_dim(by_owner, 1 - core, 1, keepdims=False)
    chip_sum = kept.astype(jnp.float32) + swap(given).astype(jnp.float32)
    hidden_state = residual.astype(jnp.float32) + lax.dynamic_index_in_dim(
        chip_sum, column, 0, keepdims=False
    )
    for step in range(1, columns):
        target = (column + step) % columns
        away = lax.dynamic_index_in_dim(chip_sum, target, 0, keepdims=False).astype(jnp.bfloat16)
        pairs = [(i, (i + 2 * step) % head) for i in range(head)]
        hidden_state = hidden_state + lax.ppermute(away, "head", pairs).astype(jnp.float32)
    normed = rms_normed(hidden_state, norm_gain)

    chosen = expert_ids[:, :, None] == jnp.arange(experts, dtype=jnp.int32)
    dense = jnp.sum(jnp.where(chosen, route_weights[:, :, None], 0.0), 1)
    high = lax.reduce_precision(dense, 8, 7)
    middle = lax.reduce_precision(dense - high, 8, 7)
    low = dense - high - middle
    spare = -3 * experts % LANES
    coded = jnp.concatenate([high, middle, low, jnp.zeros((shard_rows, spare), jnp.float32)], 1)
    mine = jnp.concatenate([normed, coded.astype(jnp.bfloat16)], 1)

    own = jnp.concatenate([mine, swap(mine)], 0)
    expert = (lax.axis_index("seq") * columns + column).reshape(1, 1)
    terms = functools.partial(
        expert_terms,
        expert=expert,
        experts=experts,
        gate_proj=gate_proj,
        up_proj=up_proj,
        down_proj=down_proj,
    )
    own_term = None
    sums = []
    travelling = own
    for step in range(1, chips // 2):
        travelling = ring(travelling)
        other = swap(travelling)
        if step == 1:
            give, keep, own_term = terms([travelling, other, own])
        else:
            give, keep = terms([travelling, other])
        sums.append((keep, swap(give)))
    travelling = ring(travelling[:shard_rows])
    give, keep = terms([travelling, swap(travelling)])
    if own_term is None:
        (own_term,) = terms([own])
    passing = (keep.astype(jnp.float32) + swap(give).astype(jnp.float32)).astype(jnp.bfloat16)
    passing = ring(passing)
    for keep, taken in reversed(sums):
        total = keep.astype(jnp.float32) + taken.astype(jnp.float32)
        if passing.shape[0] < total.shape[0]:
            front = total[:shard_rows] + passing.astype(jnp.float32)
            total = jnp.concatenate([front, total[shard_rows:]], 0)
        else:
            total = total + passing.astype(jnp.float32)
        passing = ring(total.astype(jnp.bfloat16))
    if passing.shape[0] == shard_rows:
        passing = jnp.concatenate([passing, jnp.zeros_like(passing)], 0)
    passing = passing.astype(jnp.float32)
    own_term = own_term.astype(jnp.float32)
    away = (passing[:shard_rows] + own_term[shard_rows:]).astype(jnp.bfloat16)
    mixture = passing[shard_rows:] + own_term[:shard_rows] + swap(away).astype(jnp.float32)
    return (hidden_state + mixture).astype(jnp.bfloat16)


def per_device(
    query_states,
    key_states,
    value_states,
    sink_logits,
    segment_ids,
    residual,
    out_weight,
    norm_gain,
    expert_ids,
    route_weights,
    gate_proj,
    up_proj,
    down_proj,
):
    attended = attention(query_states, key_states, value_states, sink_logits, segment_ids)
    seq, head, pair = lax.axis_size("seq"), lax.axis_size("head"), lax.axis_size("pair")
    experts = seq * head // 2
    dense_pays = 2 * expert_ids.shape[1] >= experts
    ring_fits = pair == 1 and head % 2 == 0 and experts % 2 == 0 and 3 * experts <= LANES
    layer = ring_layer if dense_pays and ring_fits else exchanged_layer
    return layer(
        attended,
        residual,
        out_weight,
        norm_gain,
        expert_ids,
        route_weights,
        gate_proj,
        up_proj,
        down_proj,
    )


def solution(mesh):
    in_specs = (
        P(("group", "seq"), ("head", "pair")),
        P(("group", "seq"), "head"),
        P(("group", "seq"), "head"),
        P(("head", "pair")),
        P("group"),
        P(("group", "seq", "head", "pair"), None),
        P(("head", "pair"), None),
        P(),
        P(("group", "seq", "head", "pair"), None),
        P(("group", "seq", "head", "pair"), None),
        P(("seq", "head"), None, "pair"),
        P(("seq", "head"), None, "pair"),
        P(("seq", "head"), "pair", None),
    )
    out_specs = P(("group", "seq", "head", "pair"), None)
    return jax.shard_map(
        per_device, mesh=mesh, in_specs=in_specs, out_specs=out_specs, check_vma=False
    )
```

```python
import functools

import jax
import jax.numpy as jnp
from jax import lax
from jax.experimental import pallas as pl
from jax.experimental.pallas import tpu as pltpu
from jax.sharding import PartitionSpec as P


HEADS = 64
KV_HEADS = 8
HEAD_DIM = 64
WINDOW = 128
LANES = 128


def passed_along(value, axis, by):
    peers = lax.axis_size(axis)
    pairs = [(i, i + by) for i in range(peers) if 0 <= i + by < peers]
    return lax.ppermute(value, axis, pairs)


def partner(value, axis, distance):
    return lax.ppermute(value, axis, [(i, i ^ 1 << distance) for i in range(lax.axis_size(axis))])


def round_keep(values):
    return lax.optimization_barrier(values.astype(jnp.bfloat16)).astype(jnp.float32)


def window_attention(
    query_block, key_block, value_block, query_pos, key_pos, query_seg, key_seg, sink_logits
):
    scores = jnp.einsum(
        "qhd,khd->hqk", query_block, key_block, preferred_element_type=jnp.float32
    ) * HEAD_DIM ** (-0.5)
    visible = (key_pos[None, :] <= query_pos[:, None]) & (
        query_pos[:, None] - key_pos[None, :] < WINDOW
    )
    visible = visible & (key_pos[None, :] >= 0) & (key_seg[None, :] == query_seg[:, None])
    masked = jnp.where(visible[None], scores, -1e30)
    row_max = jnp.maximum(jnp.max(masked, -1), sink_logits[:, None])
    weights_exp = jnp.exp(masked - row_max[..., None])
    denominator = jnp.sum(weights_exp, -1) + jnp.exp(sink_logits[:, None] - row_max)
    probs = (weights_exp / denominator[..., None]).astype(jnp.bfloat16)
    attended = jnp.einsum("hqk,khd->qhd", probs, value_block, preferred_element_type=jnp.float32)
    return attended.astype(jnp.bfloat16)


def attention(query_states, key_states, value_states, sink_logits, segment_ids):
    tok_rows = query_states.shape[0]
    local_heads = query_states.shape[1] // HEAD_DIM
    local_groups = key_states.shape[1] // HEAD_DIM
    group_size = HEADS // KV_HEADS
    tail_keys, tail_values = passed_along(
        (key_states[tok_rows - WINDOW :], value_states[tok_rows - WINDOW :]), "seq", 1
    )
    ext_keys = jnp.concatenate([tail_keys, key_states], 0).reshape(
        tok_rows + WINDOW, local_groups, HEAD_DIM
    )
    ext_values = jnp.concatenate([tail_values, value_states], 0).reshape(
        tok_rows + WINDOW, local_groups, HEAD_DIM
    )
    kv_owner = (
        lax.axis_index("pair") * local_heads + jnp.arange(local_heads, dtype=jnp.int32)
    ) // group_size
    head_select = (kv_owner[:, None] == jnp.arange(local_groups, dtype=jnp.int32)[None, :]).astype(
        jnp.bfloat16
    )
    keys_per_head = jnp.einsum(
        "kcd,hc->khd", ext_keys, head_select, preferred_element_type=jnp.float32
    ).astype(jnp.bfloat16)
    values_per_head = jnp.einsum(
        "kcd,hc->khd", ext_values, head_select, preferred_element_type=jnp.float32
    ).astype(jnp.bfloat16)
    query_heads = query_states.reshape(tok_rows, local_heads, HEAD_DIM)
    seq_start = lax.axis_index("seq") * tok_rows
    seg_padded = jnp.concatenate([jnp.full((WINDOW,), -1, jnp.int32), segment_ids], 0)
    block_rows = min(512, tok_rows)

    def attend(block_index):
        first_row = block_index * block_rows
        query_pos = seq_start + first_row + jnp.arange(block_rows, dtype=jnp.int32)
        key_pos = seq_start + first_row - WINDOW + jnp.arange(block_rows + WINDOW, dtype=jnp.int32)
        query_seg = lax.dynamic_slice_in_dim(segment_ids, seq_start + first_row, block_rows, 0)
        key_seg = lax.dynamic_slice_in_dim(
            seg_padded, seq_start + first_row, block_rows + WINDOW, 0
        )
        return window_attention(
            query_heads,
            keys_per_head,
            values_per_head,
            query_pos,
            key_pos,
            query_seg,
            key_seg,
            sink_logits,
        )

    attended = lax.map(attend, jnp.arange(tok_rows // block_rows, dtype=jnp.int32))
    return attended.reshape(tok_rows, local_heads * HEAD_DIM)


def rms_normed(hidden_state, norm_gain):
    variance = jnp.mean(hidden_state * hidden_state, -1, keepdims=True)
    return (hidden_state * lax.rsqrt(variance + 1e-05) * norm_gain).astype(jnp.bfloat16)


def exchanged_layer(
    attended,
    residual,
    out_weight,
    norm_gain,
    expert_ids,
    route_weights,
    gate_proj,
    up_proj,
    down_proj,
):
    shard_rows = residual.shape[0]
    width = residual.shape[1]
    projected = lax.psum_scatter(
        round_keep(jnp.dot(attended, out_weight, preferred_element_type=jnp.float32)).astype(
            jnp.bfloat16
        ),
        ("head", "pair"),
        scatter_dimension=0,
        tiled=True,
    ).astype(jnp.float32)
    hidden_state = residual.astype(jnp.float32) + projected
    normed = rms_normed(hidden_state, norm_gain)
    top_count = expert_ids.shape[1]
    experts = lax.axis_size("seq") * lax.axis_size("head") // 2
    capacity = min(shard_rows, max(2, 3 * shard_rows * top_count // (2 * experts)))
    flat_ids = expert_ids.reshape(-1)
    onehot = (flat_ids[:, None] == jnp.arange(experts, dtype=jnp.int32)[None, :]).astype(jnp.int32)
    before = jnp.cumsum(onehot, axis=0, dtype=jnp.int32) - onehot
    slot_rank = jnp.sum(before * onehot, -1)
    slot_index = flat_ids * capacity + slot_rank
    dispatch_mat = (
        slot_index[None, :] == jnp.arange(experts * capacity, dtype=jnp.int32)[:, None]
    ).astype(jnp.bfloat16)
    repeated = jnp.repeat(normed, top_count, axis=0)
    outgoing = jnp.dot(dispatch_mat, repeated, preferred_element_type=jnp.float32).astype(
        jnp.bfloat16
    )
    outgoing = outgoing.reshape(experts, capacity, width)
    half_idx = lax.axis_index("head") % 2
    half_width = width // 2
    split_rows = outgoing.reshape(experts, capacity, 2, half_width).transpose(0, 2, 1, 3)
    split_rows = split_rows.reshape(2 * experts, capacity, half_width)
    own_half = lax.all_to_all(split_rows, ("seq", "head"), split_axis=0, concat_axis=0, tiled=True)
    other_half = partner(own_half, "head", 0)
    arrived = jnp.where(
        half_idx == 0,
        jnp.concatenate([own_half, other_half], -1),
        jnp.concatenate([other_half, own_half], -1),
    )
    piece_rows = lax.all_gather(arrived, "pair", axis=0, tiled=True)
    flat_rows = piece_rows.reshape(-1, width)
    gate_val = jnp.minimum(
        jnp.dot(flat_rows, gate_proj[0], preferred_element_type=jnp.float32), 7.0
    )
    up_val = jnp.clip(
        jnp.dot(flat_rows, up_proj[0], preferred_element_type=jnp.float32), -7.0, 7.0
    )
    activated = ((up_val + 1.0) * gate_val * jax.nn.sigmoid(1.702 * gate_val)).astype(jnp.bfloat16)
    partial_value = round_keep(jnp.dot(activated, down_proj[0], preferred_element_type=jnp.float32))
    quarter_terms = partial_value.reshape(piece_rows.shape)
    pair_sums = lax.psum_scatter(
        quarter_terms.astype(jnp.bfloat16), "pair", scatter_dimension=0, tiled=True
    ).astype(jnp.float32)
    kept_half = lax.dynamic_slice_in_dim(pair_sums, half_idx * half_width, half_width, 2)
    given_half = lax.dynamic_slice_in_dim(pair_sums, (1 - half_idx) * half_width, half_width, 2)
    partner_half = partner(given_half.astype(jnp.bfloat16), "head", 0).astype(given_half.dtype)
    merged = kept_half + partner_half
    returned = lax.all_to_all(
        merged.astype(jnp.bfloat16), ("seq", "head"), split_axis=0, concat_axis=0, tiled=True
    ).astype(merged.dtype)
    expert_out = (
        returned.reshape(experts, 2, capacity, half_width)
        .transpose(0, 2, 1, 3)
        .reshape(experts, capacity, width)
    )
    slot_table = slot_index.reshape(shard_rows, top_count)
    columns_all = jnp.arange(experts * capacity, dtype=jnp.int32)
    combine_mat = jnp.sum(
        jnp.where(
            slot_table[:, :, None] == columns_all[None, None, :], route_weights[:, :, None], 0.0
        ),
        axis=1,
    )
    mixture = jnp.dot(
        combine_mat, expert_out.reshape(experts * capacity, width), precision=lax.Precision.HIGHEST
    )
    return (hidden_state + mixture).astype(jnp.bfloat16)


def attend_block(
    query, window_keys, window_values, bias, sink_ref, score_ref, prob_ref, inverse_ref, store
):
    rows = query.shape[0]
    span = window_keys.shape[0]
    groups = window_keys.shape[1] // HEAD_DIM
    tiles = query.shape[1] // LANES // groups
    lane = lax.broadcasted_iota(jnp.int32, (span, LANES), 1)
    out_lane = lax.broadcasted_iota(jnp.int32, (rows, LANES), 1)

    def both_sides(values, group):
        tile = values[:, group // 2 * LANES : (group // 2 + 1) * LANES]
        here = jnp.where(lane // HEAD_DIM == group % 2, tile, 0.0)
        there = pltpu.roll(here, HEAD_DIM, 1)
        sides = [here, there] if group % 2 == 0 else [there, here]
        return jnp.concatenate(sides, 0).astype(jnp.bfloat16)

    for group in range(groups):
        keys = both_sides(window_keys.astype(jnp.float32) * HEAD_DIM**-0.5, group)
        first = group * tiles
        stacked = jnp.concatenate(
            [query[:, (first + t) * LANES : (first + t + 1) * LANES] for t in range(tiles)], 0
        )
        score_ref[group] = lax.dot_general(
            stacked, keys, (((1,), (1,)), ((), ())), preferred_element_type=jnp.float32
        )
    for group in range(groups):
        first = group * tiles
        for t in range(tiles):
            at = slice(t * rows, (t + 1) * rows)
            inverses = []
            for side in range(2):
                cols = slice(side * span, (side + 1) * span)
                sink = sink_ref[2 * (first + t) + side]
                masked = score_ref[group, at, cols] + bias
                top = jnp.maximum(jnp.max(masked, -1, keepdims=True), sink)
                weights = jnp.exp(masked - top)
                total = jnp.sum(weights, -1, keepdims=True) + jnp.exp(sink - top)
                prob_ref[group, at, cols] = weights.astype(jnp.bfloat16)
                inverses.append(1.0 / total)
            inverse_ref[group, at, :] = jnp.where(out_lane < HEAD_DIM, inverses[0], inverses[1])
    for group in range(groups):
        first = group * tiles
        values = both_sides(window_values.astype(jnp.float32), group)
        out = jnp.dot(prob_ref[group], values, preferred_element_type=jnp.float32)
        out = (out * inverse_ref[group]).astype(jnp.bfloat16)
        for t in range(tiles):
            store(first + t, out[t * rows : (t + 1) * rows])


def visible_bias(segment_ref, before, here, starts):
    row = segment_ref[pl.ds(here, 1), :]
    prior = jnp.where(starts, -1, segment_ref[pl.ds(before, 1), :])
    block = (WINDOW, WINDOW)
    own = jnp.transpose(jnp.broadcast_to(row, block).astype(jnp.float32))
    query_at = lax.broadcasted_iota(jnp.int32, block, 0)
    key_at = lax.broadcasted_iota(jnp.int32, block, 1)
    earlier = (key_at > query_at) & (own == prior.astype(jnp.float32))
    later = (key_at <= query_at) & (own == row.astype(jnp.float32))
    seen = jnp.concatenate([earlier, later], 1)
    return jnp.where(seen, 0.0, -1e30)


def later_body(seq_ref, sink_ref, query_ref, key_ref, value_ref, segment_ref, out_ref, *scratch):
    blocks = query_ref.shape[0] // WINDOW
    for block in range(1, blocks):
        here = seq_ref[0] * blocks + block
        bias = visible_bias(segment_ref, here - 1, here, False)
        rows = slice(block * WINDOW, (block + 1) * WINDOW)
        window = slice((block - 1) * WINDOW, (block + 1) * WINDOW)

        def store(tile, value, block=block):
            at = slice((block - 1) * WINDOW, block * WINDOW)
            out_ref[at, tile * LANES : (tile + 1) * LANES] = value

        attend_block(
            query_ref[rows, :],
            key_ref[window, :],
            value_ref[window, :],
            bias,
            sink_ref,
            *scratch,
            store,
        )


def first_body(
    seq_ref,
    sink_ref,
    query_ref,
    key_ref,
    value_ref,
    segment_ref,
    tail_ref,
    later_ref,
    weight_ref,
    kept_ref,
    given_ref,
    sorted_ref,
    *scratch,
):
    tokens = later_ref.shape[0] + WINDOW
    half = tokens // 2
    shard_rows = kept_ref.shape[1]
    piece = min(shard_rows, WINDOW)
    core = seq_ref[1]
    blocks = tokens // WINDOW
    here = seq_ref[0] * blocks
    starts = seq_ref[0] == 0
    bias = visible_bias(segment_ref, jnp.maximum(here - 1, 0), here, starts)
    kv_width = key_ref.shape[1]

    def goal(row):
        owner = row // shard_rows
        side = jnp.where(core == owner % 2, 0, half)
        return pl.multiple_of(side + owner // 2 * shard_rows + row % shard_rows, piece)

    for row in range(WINDOW, tokens, piece):
        sorted_ref[pl.ds(goal(row), piece), :] = later_ref[row - WINDOW : row - WINDOW + piece, :]

    def store(tile, value):
        for row in range(0, WINDOW, piece):
            sorted_ref[pl.ds(goal(row), piece), tile * LANES : (tile + 1) * LANES] = value[
                row : row + piece
            ]

    attend_block(
        query_ref[...],
        jnp.concatenate([tail_ref[:, :kv_width], key_ref[...]], 0),
        jnp.concatenate([tail_ref[:, kv_width:], value_ref[...]], 0),
        bias,
        sink_ref,
        *scratch,
        store,
    )
    width = weight_ref.shape[1]
    columns = kept_ref.shape[0]
    tile = 512 if width % 512 == 0 else width
    for low in range(0, width, tile):
        cols = slice(low, low + tile)
        value = jnp.dot(
            sorted_ref[...], weight_ref[:, cols], preferred_element_type=jnp.float32
        ).astype(jnp.bfloat16)
        for column in range(columns):
            at = column * shard_rows
            kept_ref[column, :, cols] = value[at : at + shard_rows]
            given_ref[column, :, cols] = value[half + at : half + at + shard_rows]


VMEM = pl.BlockSpec(memory_space=pltpu.VMEM)
SMEM = pl.BlockSpec(memory_space=pltpu.SMEM)


def call(body, outs, args, specs, scratch=(), flops=0, limit=16 << 20):
    moved = sum(a.size * a.dtype.itemsize for a in args)
    return pl.pallas_call(
        body,
        out_shape=outs,
        in_specs=specs,
        out_specs=jax.tree.map(lambda _: VMEM, outs),
        scratch_shapes=list(scratch),
        compiler_params=pltpu.CompilerParams(vmem_limit_bytes=limit),
        cost_estimate=pl.CostEstimate(flops=flops, bytes_accessed=moved, transcendentals=0),
    )(*args)


def projected_heads(
    query_states, key_states, value_states, sink_logits, segment_ids, out_weight, shard_rows
):
    tokens, width = query_states.shape
    kv_width = key_states.shape[1]
    groups = kv_width // HEAD_DIM
    stack = width // LANES // groups * WINDOW
    where_at = jnp.stack([lax.axis_index("seq"), lax.axis_index("head") % 2]).astype(jnp.int32)
    segment_rows = segment_ids.reshape(-1, WINDOW)
    tail = passed_along(
        jnp.concatenate([key_states[tokens - WINDOW :], value_states[tokens - WINDOW :]], 1),
        "seq",
        1,
    )
    scratch = [
        pltpu.VMEM((groups, stack, 4 * WINDOW), jnp.float32),
        pltpu.VMEM((groups, stack, 4 * WINDOW), jnp.bfloat16),
        pltpu.VMEM((groups, stack, LANES), jnp.float32),
    ]
    flops = 16 * WINDOW * WINDOW * width
    later = call(
        later_body,
        jax.ShapeDtypeStruct((tokens - WINDOW, width), jnp.bfloat16),
        [where_at, sink_logits, query_states, key_states, value_states, segment_rows],
        [SMEM, SMEM] + [VMEM] * 4,
        scratch,
        flops * (tokens // WINDOW - 1),
    )
    columns = tokens // (2 * shard_rows)
    out_width = out_weight.shape[1]
    side = jax.ShapeDtypeStruct((columns, shard_rows, out_width), jnp.bfloat16)
    return call(
        first_body,
        [side, side],
        [
            where_at,
            sink_logits,
            query_states[:WINDOW],
            key_states[:WINDOW],
            value_states[:WINDOW],
            segment_rows,
            tail,
            later,
            out_weight,
        ],
        [SMEM, SMEM] + [VMEM] * 7,
        [pltpu.VMEM((tokens, width), jnp.bfloat16)] + scratch,
        flops + 2 * tokens * width * out_width,
        24 << 20,
    )


def chip_body(at_ref, kept_ref, taken_ref, residual_ref, hidden_ref, *away_refs):
    columns = kept_ref.shape[0]
    column = at_ref[0]
    total = kept_ref[column].astype(jnp.float32) + taken_ref[column].astype(jnp.float32)
    hidden_ref[...] = residual_ref[...].astype(jnp.float32) + total
    for step, away_ref in enumerate(away_refs):
        target = lax.rem(column + step + 1, columns)
        total = kept_ref[target].astype(jnp.float32) + taken_ref[target].astype(jnp.float32)
        away_ref[...] = total.astype(away_ref.dtype)


def norm_body(count, experts, partial_ref, gain_ref, ids_ref, route_ref, *refs):
    arrived = refs[:count]
    hidden_ref, packed_ref = refs[count:]
    hidden = partial_ref[...]
    for ref in arrived:
        hidden = hidden + ref[...].astype(jnp.float32)
    hidden_ref[...] = hidden
    width = hidden.shape[1]
    variance = jnp.mean(hidden * hidden, -1, keepdims=True)
    normed = hidden * lax.rsqrt(variance + 1e-05) * gain_ref[...]
    packed_ref[:, :width] = normed.astype(packed_ref.dtype)
    lane = lax.broadcasted_iota(jnp.int32, (hidden.shape[0], LANES), 1)
    name = lax.rem(lane, experts)
    dense = jnp.zeros((hidden.shape[0], LANES), jnp.float32)
    for choice in range(ids_ref.shape[1]):
        ids = ids_ref[:, choice : choice + 1]
        dense = dense + jnp.where(ids == name, route_ref[:, choice : choice + 1], 0.0)
    high = dense.astype(jnp.bfloat16)
    rest = dense - high.astype(jnp.float32)
    middle = rest.astype(jnp.bfloat16)
    low = (rest - middle.astype(jnp.float32)).astype(jnp.bfloat16)
    third = lane // experts
    coded = jnp.where(
        third == 0,
        high.astype(jnp.float32),
        jnp.where(
            third == 1,
            middle.astype(jnp.float32),
            jnp.where(third == 2, low.astype(jnp.float32), 0.0),
        ),
    )
    packed_ref[:, width:] = coded.astype(packed_ref.dtype)


def ffn_body(experts, expert_ref, gate_ref, up_ref, down_ref, *refs):
    ins, (keep_ref, give_ref, rows_ref, act_ref) = refs[:-4], refs[-4:]
    width, hidden = gate_ref.shape[1], gate_ref.shape[2]
    half = keep_ref.shape[0]
    expert = expert_ref[0]
    scales = []
    start = 0
    for ref in ins:
        count = ref.shape[0]
        rows_ref[start : start + count, :] = ref[:, :width]
        coded = ref[:, width:].astype(jnp.float32)
        lane = lax.broadcasted_iota(jnp.int32, coded.shape, 1)
        mine = (lane == expert) | (lane == expert + experts) | (lane == expert + 2 * experts)
        scales.append(jnp.sum(jnp.where(mine, coded, 0.0), -1, keepdims=True))
        start += count
    scale = jnp.concatenate(scales, 0)
    tile = 256 if hidden % 256 == 0 else hidden
    for low in range(0, hidden, tile):
        cols = slice(low, low + tile)
        gate_val = jnp.minimum(
            jnp.dot(rows_ref[...], gate_ref[0, :, cols], preferred_element_type=jnp.float32), 7.0
        )
        up_val = jnp.clip(
            jnp.dot(rows_ref[...], up_ref[0, :, cols], preferred_element_type=jnp.float32),
            -7.0,
            7.0,
        )
        act_ref[:, cols] = ((up_val + 1.0) * gate_val * jax.nn.sigmoid(1.702 * gate_val)).astype(
            act_ref.dtype
        )
    tile = 512 if width % 512 == 0 else width
    for low in range(0, width, tile):
        cols = slice(low, low + tile)
        value = jnp.dot(act_ref[...], down_ref[0, :, cols], preferred_element_type=jnp.float32)
        value = (value * scale).astype(keep_ref.dtype)
        keep_ref[:, cols] = value[:half]
        give_ref[:, cols] = value[half:]


def ring_layer(
    query_states,
    key_states,
    value_states,
    sink_logits,
    segment_ids,
    residual,
    out_weight,
    norm_gain,
    expert_ids,
    route_weights,
    gate_proj,
    up_proj,
    down_proj,
):
    shard_rows, width = residual.shape
    hidden_units = gate_proj.shape[2]
    seq, head = lax.axis_size("seq"), lax.axis_size("head")
    columns = head // 2
    chips = seq * columns
    column = lax.axis_index("head") // 2

    order = [
        (col, row if col % 2 == 0 else seq - 1 - row) for col in range(columns) for row in range(seq)
    ]

    def device(place, which):
        col, row = order[place % chips]
        return row * head + col * 2 + which

    onward = [(device(p, c), device(p + 1, c)) for p in range(chips) for c in range(2)]
    back = [(b, a) for a, b in onward]

    def ring(pair):
        on = lax.ppermute(pair[0], ("seq", "head"), onward)
        off = lax.ppermute(pair[1], ("seq", "head"), back)
        return on, off

    def swap(value):
        return partner(value, "head", 0)

    kept, given = projected_heads(
        query_states, key_states, value_states, sink_logits, segment_ids, out_weight, shard_rows
    )
    rows_f32 = jax.ShapeDtypeStruct((shard_rows, width), jnp.float32)
    rows_bf16 = jax.ShapeDtypeStruct((shard_rows, width), jnp.bfloat16)
    hidden_state, *away = call(
        chip_body,
        [rows_f32] + [rows_bf16] * (columns - 1),
        [column.reshape(1), kept, swap(given), residual],
        [SMEM] + [VMEM] * 3,
    )
    arrived = []
    for step, value in enumerate(away):
        pairs = [(i, (i + 2 * (step + 1)) % head) for i in range(head)]
        arrived.append(lax.ppermute(value, "head", pairs))
    packed_width = width + LANES
    hidden_state, mine = call(
        functools.partial(norm_body, len(arrived), chips),
        [rows_f32, jax.ShapeDtypeStruct((shard_rows, packed_width), jnp.bfloat16)],
        [hidden_state, norm_gain.reshape(1, -1), expert_ids, route_weights] + arrived,
        [VMEM] * (4 + len(arrived)),
    )

    expert = (lax.axis_index("seq") * columns + column).reshape(1)

    def terms(blocks):
        rows = 2 * sum(block.shape[0] for block in blocks)
        others = [swap(block) for block in blocks]
        out = jax.ShapeDtypeStruct((rows // 2, width), jnp.bfloat16)
        keep, give = call(
            functools.partial(ffn_body, chips),
            [out, out],
            [expert, gate_proj, up_proj, down_proj] + blocks + others,
            [SMEM] + [VMEM] * (3 + 2 * len(blocks)),
            [
                pltpu.VMEM((rows, width), jnp.bfloat16),
                pltpu.VMEM((rows, hidden_units), jnp.bfloat16),
            ],
            6 * rows * width * hidden_units,
            24 << 20,
        )
        taken = swap(give)
        return keep.astype(jnp.float32) + taken.astype(jnp.float32)

    half = shard_rows // 2
    own_term = terms([mine])
    sums = []
    travelling = (mine, mine)
    for _ in range(1, chips // 2):
        travelling = ring(travelling)
        sums.append(terms(list(travelling)))
    travelling = ring((travelling[0][:half], travelling[1][half:]))
    total = terms(list(travelling)).astype(jnp.bfloat16)
    passing = ring((total[:half], total[half:]))
    for total in reversed(sums):
        on, off = (value.astype(jnp.float32) for value in passing)
        if on.shape[0] < shard_rows:
            on = jnp.pad(on, ((0, half), (0, 0)))
            off = jnp.pad(off, ((half, 0), (0, 0)))
        on = (total[shard_rows:] + on).astype(jnp.bfloat16)
        off = (total[:shard_rows] + off).astype(jnp.bfloat16)
        passing = ring((on, off))
    on, off = (value.astype(jnp.float32) for value in passing)
    if on.shape[0] < shard_rows:
        on = jnp.concatenate([on, off], 0)
        off = 0.0
    return (hidden_state + (on + off + own_term)).astype(jnp.bfloat16)


def per_device(query_states, key_states, value_states, sink_logits, segment_ids, *rest):
    residual, _, _, expert_ids = rest[:4]
    seq, head, pair = lax.axis_size("seq"), lax.axis_size("head"), lax.axis_size("pair")
    experts = seq * head // 2
    dense_pays = 2 * expert_ids.shape[1] >= experts
    ring_fits = pair == 1 and head % 2 == 0 and experts % 2 == 0 and 3 * experts <= LANES
    shard_rows = residual.shape[0]
    tokens, width = query_states.shape
    kv_width = key_states.shape[1]
    rows_fit = shard_rows % 32 == 0 and tokens % WINDOW == 0 and WINDOW % min(shard_rows, WINDOW) == 0
    heads_fit = kv_width % LANES == 0 and width % (2 * kv_width) == 0
    if dense_pays and ring_fits and rows_fit and heads_fit:
        return ring_layer(query_states, key_states, value_states, sink_logits, segment_ids, *rest)
    attended = attention(query_states, key_states, value_states, sink_logits, segment_ids)
    return exchanged_layer(attended, *rest)


def solution(mesh):
    in_specs = (
        P(("group", "seq"), ("head", "pair")),
        P(("group", "seq"), "head"),
        P(("group", "seq"), "head"),
        P(("head", "pair")),
        P("group"),
        P(("group", "seq", "head", "pair"), None),
        P(("head", "pair"), None),
        P(),
        P(("group", "seq", "head", "pair"), None),
        P(("group", "seq", "head", "pair"), None),
        P(("seq", "head"), None, "pair"),
        P(("seq", "head"), None, "pair"),
        P(("seq", "head"), "pair", None),
    )
    out_specs = P(("group", "seq", "head", "pair"), None)
    return jax.shard_map(
        per_device, mesh=mesh, in_specs=in_specs, out_specs=out_specs, check_vma=False
    )
```

```python
import functools

import jax
import jax.numpy as jnp
from jax import lax
from jax.experimental import pallas as pl
from jax.experimental.pallas import tpu as pltpu
from jax.sharding import PartitionSpec as P


HEADS = 64
KV_HEADS = 8
HEAD_DIM = 64
WINDOW = 128
LANES = 128


def passed_along(value, axis, by):
    peers = lax.axis_size(axis)
    pairs = [(i, i + by) for i in range(peers) if 0 <= i + by < peers]
    return lax.ppermute(value, axis, pairs)


def partner(value, axis, distance):
    return lax.ppermute(value, axis, [(i, i ^ 1 << distance) for i in range(lax.axis_size(axis))])


def round_keep(values):
    return lax.optimization_barrier(values.astype(jnp.bfloat16)).astype(jnp.float32)


def window_attention(
    query_block, key_block, value_block, query_pos, key_pos, query_seg, key_seg, sink_logits
):
    scores = jnp.einsum(
        "qhd,khd->hqk", query_block, key_block, preferred_element_type=jnp.float32
    ) * HEAD_DIM ** (-0.5)
    visible = (key_pos[None, :] <= query_pos[:, None]) & (
        query_pos[:, None] - key_pos[None, :] < WINDOW
    )
    visible = visible & (key_pos[None, :] >= 0) & (key_seg[None, :] == query_seg[:, None])
    masked = jnp.where(visible[None], scores, -1e30)
    row_max = jnp.maximum(jnp.max(masked, -1), sink_logits[:, None])
    weights_exp = jnp.exp(masked - row_max[..., None])
    denominator = jnp.sum(weights_exp, -1) + jnp.exp(sink_logits[:, None] - row_max)
    probs = (weights_exp / denominator[..., None]).astype(jnp.bfloat16)
    attended = jnp.einsum("hqk,khd->qhd", probs, value_block, preferred_element_type=jnp.float32)
    return attended.astype(jnp.bfloat16)


def attention(query_states, key_states, value_states, sink_logits, segment_ids):
    tok_rows = query_states.shape[0]
    local_heads = query_states.shape[1] // HEAD_DIM
    local_groups = key_states.shape[1] // HEAD_DIM
    group_size = HEADS // KV_HEADS
    tail_keys, tail_values = passed_along(
        (key_states[tok_rows - WINDOW :], value_states[tok_rows - WINDOW :]), "seq", 1
    )
    ext_keys = jnp.concatenate([tail_keys, key_states], 0).reshape(
        tok_rows + WINDOW, local_groups, HEAD_DIM
    )
    ext_values = jnp.concatenate([tail_values, value_states], 0).reshape(
        tok_rows + WINDOW, local_groups, HEAD_DIM
    )
    kv_owner = (
        lax.axis_index("pair") * local_heads + jnp.arange(local_heads, dtype=jnp.int32)
    ) // group_size
    head_select = (kv_owner[:, None] == jnp.arange(local_groups, dtype=jnp.int32)[None, :]).astype(
        jnp.bfloat16
    )
    keys_per_head = jnp.einsum(
        "kcd,hc->khd", ext_keys, head_select, preferred_element_type=jnp.float32
    ).astype(jnp.bfloat16)
    values_per_head = jnp.einsum(
        "kcd,hc->khd", ext_values, head_select, preferred_element_type=jnp.float32
    ).astype(jnp.bfloat16)
    query_heads = query_states.reshape(tok_rows, local_heads, HEAD_DIM)
    seq_start = lax.axis_index("seq") * tok_rows
    seg_padded = jnp.concatenate([jnp.full((WINDOW,), -1, jnp.int32), segment_ids], 0)
    block_rows = min(512, tok_rows)

    def attend(block_index):
        first_row = block_index * block_rows
        query_pos = seq_start + first_row + jnp.arange(block_rows, dtype=jnp.int32)
        key_pos = seq_start + first_row - WINDOW + jnp.arange(block_rows + WINDOW, dtype=jnp.int32)
        query_seg = lax.dynamic_slice_in_dim(segment_ids, seq_start + first_row, block_rows, 0)
        key_seg = lax.dynamic_slice_in_dim(
            seg_padded, seq_start + first_row, block_rows + WINDOW, 0
        )
        return window_attention(
            query_heads,
            keys_per_head,
            values_per_head,
            query_pos,
            key_pos,
            query_seg,
            key_seg,
            sink_logits,
        )

    attended = lax.map(attend, jnp.arange(tok_rows // block_rows, dtype=jnp.int32))
    return attended.reshape(tok_rows, local_heads * HEAD_DIM)


def rms_normed(hidden_state, norm_gain):
    variance = jnp.mean(hidden_state * hidden_state, -1, keepdims=True)
    return (hidden_state * lax.rsqrt(variance + 1e-05) * norm_gain).astype(jnp.bfloat16)


def exchanged_layer(
    attended,
    residual,
    out_weight,
    norm_gain,
    expert_ids,
    route_weights,
    gate_proj,
    up_proj,
    down_proj,
):
    shard_rows = residual.shape[0]
    width = residual.shape[1]
    projected = lax.psum_scatter(
        round_keep(jnp.dot(attended, out_weight, preferred_element_type=jnp.float32)).astype(
            jnp.bfloat16
        ),
        ("head", "pair"),
        scatter_dimension=0,
        tiled=True,
    ).astype(jnp.float32)
    hidden_state = residual.astype(jnp.float32) + projected
    normed = rms_normed(hidden_state, norm_gain)
    top_count = expert_ids.shape[1]
    experts = lax.axis_size("seq") * lax.axis_size("head") // 2
    capacity = min(shard_rows, max(2, 3 * shard_rows * top_count // (2 * experts)))
    flat_ids = expert_ids.reshape(-1)
    onehot = (flat_ids[:, None] == jnp.arange(experts, dtype=jnp.int32)[None, :]).astype(jnp.int32)
    before = jnp.cumsum(onehot, axis=0, dtype=jnp.int32) - onehot
    slot_rank = jnp.sum(before * onehot, -1)
    slot_index = flat_ids * capacity + slot_rank
    dispatch_mat = (
        slot_index[None, :] == jnp.arange(experts * capacity, dtype=jnp.int32)[:, None]
    ).astype(jnp.bfloat16)
    repeated = jnp.repeat(normed, top_count, axis=0)
    outgoing = jnp.dot(dispatch_mat, repeated, preferred_element_type=jnp.float32).astype(
        jnp.bfloat16
    )
    outgoing = outgoing.reshape(experts, capacity, width)
    half_idx = lax.axis_index("head") % 2
    half_width = width // 2
    split_rows = outgoing.reshape(experts, capacity, 2, half_width).transpose(0, 2, 1, 3)
    split_rows = split_rows.reshape(2 * experts, capacity, half_width)
    own_half = lax.all_to_all(split_rows, ("seq", "head"), split_axis=0, concat_axis=0, tiled=True)
    other_half = partner(own_half, "head", 0)
    arrived = jnp.where(
        half_idx == 0,
        jnp.concatenate([own_half, other_half], -1),
        jnp.concatenate([other_half, own_half], -1),
    )
    piece_rows = lax.all_gather(arrived, "pair", axis=0, tiled=True)
    flat_rows = piece_rows.reshape(-1, width)
    gate_val = jnp.minimum(
        jnp.dot(flat_rows, gate_proj[0], preferred_element_type=jnp.float32), 7.0
    )
    up_val = jnp.clip(
        jnp.dot(flat_rows, up_proj[0], preferred_element_type=jnp.float32), -7.0, 7.0
    )
    activated = ((up_val + 1.0) * gate_val * jax.nn.sigmoid(1.702 * gate_val)).astype(jnp.bfloat16)
    partial_value = round_keep(jnp.dot(activated, down_proj[0], preferred_element_type=jnp.float32))
    quarter_terms = partial_value.reshape(piece_rows.shape)
    pair_sums = lax.psum_scatter(
        quarter_terms.astype(jnp.bfloat16), "pair", scatter_dimension=0, tiled=True
    ).astype(jnp.float32)
    kept_half = lax.dynamic_slice_in_dim(pair_sums, half_idx * half_width, half_width, 2)
    given_half = lax.dynamic_slice_in_dim(pair_sums, (1 - half_idx) * half_width, half_width, 2)
    partner_half = partner(given_half.astype(jnp.bfloat16), "head", 0).astype(given_half.dtype)
    merged = kept_half + partner_half
    returned = lax.all_to_all(
        merged.astype(jnp.bfloat16), ("seq", "head"), split_axis=0, concat_axis=0, tiled=True
    ).astype(merged.dtype)
    expert_out = (
        returned.reshape(experts, 2, capacity, half_width)
        .transpose(0, 2, 1, 3)
        .reshape(experts, capacity, width)
    )
    slot_table = slot_index.reshape(shard_rows, top_count)
    columns_all = jnp.arange(experts * capacity, dtype=jnp.int32)
    combine_mat = jnp.sum(
        jnp.where(
            slot_table[:, :, None] == columns_all[None, None, :], route_weights[:, :, None], 0.0
        ),
        axis=1,
    )
    mixture = jnp.dot(
        combine_mat, expert_out.reshape(experts * capacity, width), precision=lax.Precision.HIGHEST
    )
    return (hidden_state + mixture).astype(jnp.bfloat16)


def attend_block(
    query, window_keys, window_values, bias, sink_ref, score_ref, prob_ref, inverse_ref, store
):
    rows = query.shape[0]
    span = window_keys.shape[0]
    groups = window_keys.shape[1] // HEAD_DIM
    tiles = query.shape[1] // LANES // groups
    lane = lax.broadcasted_iota(jnp.int32, (span, LANES), 1)
    out_lane = lax.broadcasted_iota(jnp.int32, (rows, LANES), 1)

    def both_sides(values, group):
        tile = values[:, group // 2 * LANES : (group // 2 + 1) * LANES]
        here = jnp.where(lane // HEAD_DIM == group % 2, tile, 0.0)
        there = pltpu.roll(here, HEAD_DIM, 1)
        sides = [here, there] if group % 2 == 0 else [there, here]
        return jnp.concatenate(sides, 0).astype(jnp.bfloat16)

    for group in range(groups):
        keys = both_sides(window_keys.astype(jnp.float32) * HEAD_DIM**-0.5, group)
        first = group * tiles
        stacked = jnp.concatenate(
            [query[:, (first + t) * LANES : (first + t + 1) * LANES] for t in range(tiles)], 0
        )
        score_ref[group] = lax.dot_general(
            stacked, keys, (((1,), (1,)), ((), ())), preferred_element_type=jnp.float32
        )
    for group in range(groups):
        first = group * tiles
        for t in range(tiles):
            at = slice(t * rows, (t + 1) * rows)
            inverses = []
            for side in range(2):
                cols = slice(side * span, (side + 1) * span)
                sink = sink_ref[2 * (first + t) + side]
                masked = score_ref[group, at, cols] + bias
                top = jnp.maximum(jnp.max(masked, -1, keepdims=True), sink)
                weights = jnp.exp(masked - top)
                total = jnp.sum(weights, -1, keepdims=True) + jnp.exp(sink - top)
                prob_ref[group, at, cols] = weights.astype(jnp.bfloat16)
                inverses.append(1.0 / total)
            inverse_ref[group, at, :] = jnp.where(out_lane < HEAD_DIM, inverses[0], inverses[1])
    for group in range(groups):
        first = group * tiles
        values = both_sides(window_values.astype(jnp.float32), group)
        out = jnp.dot(prob_ref[group], values, preferred_element_type=jnp.float32)
        out = (out * inverse_ref[group]).astype(jnp.bfloat16)
        for t in range(tiles):
            store(first + t, out[t * rows : (t + 1) * rows])


def visible_bias(segment_ref, before, here, starts):
    row = segment_ref[pl.ds(here, 1), :]
    prior = jnp.where(starts, -1, segment_ref[pl.ds(before, 1), :])
    block = (WINDOW, WINDOW)
    own = jnp.transpose(jnp.broadcast_to(row, block).astype(jnp.float32))
    query_at = lax.broadcasted_iota(jnp.int32, block, 0)
    key_at = lax.broadcasted_iota(jnp.int32, block, 1)
    earlier = (key_at > query_at) & (own == prior.astype(jnp.float32))
    later = (key_at <= query_at) & (own == row.astype(jnp.float32))
    seen = jnp.concatenate([earlier, later], 1)
    return jnp.where(seen, 0.0, -1e30)


def fetch(sources, targets, sems):
    copies = [
        pltpu.make_async_copy(source, target, sems.at[i])
        for i, (source, target) in enumerate(zip(sources, targets))
    ]
    for copy in copies:
        copy.start()
    for copy in copies:
        copy.wait()


def load_body(*refs):
    count = len(refs) // 2
    fetch(refs[:count], refs[count:-1], refs[-1])


def later_body(
    sink_any,
    query_any,
    key_any,
    value_any,
    segment_any,
    out_ref,
    tail_ref,
    sems,
    sink_ref,
    query_ref,
    key_ref,
    value_ref,
    segment_ref,
    *scratch,
):
    tokens = key_ref.shape[0]
    blocks = tokens // WINDOW
    kv_width = key_ref.shape[1]
    fetch(
        [sink_any, query_any.at[WINDOW:, :], key_any, value_any, segment_any],
        [sink_ref, query_ref, key_ref, value_ref, segment_ref],
        sems,
    )
    tail_ref[:, :kv_width] = key_ref[tokens - WINDOW :, :]
    tail_ref[:, kv_width:] = value_ref[tokens - WINDOW :, :]
    for block in range(1, blocks):
        here = lax.axis_index("seq") * blocks + block
        bias = visible_bias(segment_ref, here - 1, here, False)
        rows = slice((block - 1) * WINDOW, block * WINDOW)
        window = slice((block - 1) * WINDOW, (block + 1) * WINDOW)

        def store(tile, value, rows=rows):
            out_ref[rows, tile * LANES : (tile + 1) * LANES] = value

        attend_block(
            query_ref[rows, :],
            key_ref[window, :],
            value_ref[window, :],
            bias,
            sink_ref,
            *scratch,
            store,
        )


def first_body(
    sink_any,
    query_any,
    key_any,
    value_any,
    segment_any,
    tail_ref,
    later_ref,
    weight_ref,
    kept_ref,
    given_ref,
    sems,
    sink_ref,
    query_ref,
    key_ref,
    value_ref,
    segment_ref,
    sorted_ref,
    *scratch,
):
    tokens = later_ref.shape[0] + WINDOW
    half = tokens // 2
    shard_rows = kept_ref.shape[1]
    piece = min(shard_rows, WINDOW)
    core = lax.axis_index("head") % 2
    here = lax.axis_index("seq") * (tokens // WINDOW)
    kv_width = key_ref.shape[1]
    fetch(
        [
            sink_any,
            query_any.at[:WINDOW, :],
            key_any.at[:WINDOW, :],
            value_any.at[:WINDOW, :],
            segment_any,
        ],
        [sink_ref, query_ref, key_ref, value_ref, segment_ref],
        sems,
    )
    bias = visible_bias(segment_ref, jnp.maximum(here - 1, 0), here, here == 0)

    def goal(row):
        owner = row // shard_rows
        side = jnp.where(core == owner % 2, 0, half)
        return pl.multiple_of(side + owner // 2 * shard_rows + row % shard_rows, piece)

    for row in range(WINDOW, tokens, piece):
        sorted_ref[pl.ds(goal(row), piece), :] = later_ref[row - WINDOW : row - WINDOW + piece, :]

    def store(tile, value):
        for row in range(0, WINDOW, piece):
            sorted_ref[pl.ds(goal(row), piece), tile * LANES : (tile + 1) * LANES] = value[
                row : row + piece
            ]

    attend_block(
        query_ref[...],
        jnp.concatenate([tail_ref[:, :kv_width], key_ref[...]], 0),
        jnp.concatenate([tail_ref[:, kv_width:], value_ref[...]], 0),
        bias,
        sink_ref,
        *scratch,
        store,
    )
    width = weight_ref.shape[1]
    columns = kept_ref.shape[0]
    tile = 512 if width % 512 == 0 else width
    for low in range(0, width, tile):
        cols = slice(low, low + tile)
        value = jnp.dot(
            sorted_ref[...], weight_ref[:, cols], preferred_element_type=jnp.float32
        ).astype(jnp.bfloat16)
        for column in range(columns):
            at = column * shard_rows
            kept_ref[column, :, cols] = value[at : at + shard_rows]
            given_ref[column, :, cols] = value[half + at : half + at + shard_rows]


VMEM = pl.BlockSpec(memory_space=pltpu.VMEM)
HBM = pl.BlockSpec(memory_space=pltpu.HBM)


def call(body, outs, args, specs, scratch=(), flops=0, limit=16 << 20):
    moved = sum(a.size * a.dtype.itemsize for a in args)
    return pl.pallas_call(
        body,
        out_shape=[pltpu.VMEM(shape, dtype) for shape, dtype in outs],
        in_specs=specs,
        out_specs=[VMEM] * len(outs),
        scratch_shapes=list(scratch),
        compiler_params=pltpu.CompilerParams(vmem_limit_bytes=limit),
        cost_estimate=pl.CostEstimate(flops=flops, bytes_accessed=moved, transcendentals=0),
    )(*args)


def loaded(args):
    return call(
        load_body,
        [(a.shape, a.dtype) for a in args],
        args,
        [HBM] * len(args),
        [pltpu.SemaphoreType.DMA((len(args),))],
        limit=32 << 20,
    )


def projected_heads(
    query_states, key_states, value_states, sink_logits, segment_ids, out_weight, shard_rows
):
    tokens, width = query_states.shape
    kv_width = key_states.shape[1]
    groups = kv_width // HEAD_DIM
    stack = width // LANES // groups * WINDOW
    segment_rows = segment_ids.reshape(-1, WINDOW)
    inputs = [sink_logits, query_states, key_states, value_states, segment_rows]
    bf16, f32 = jnp.bfloat16, jnp.float32

    def local(query_rows, key_rows):
        return [
            pltpu.SemaphoreType.DMA((len(inputs),)),
            pltpu.SMEM(sink_logits.shape, f32),
            pltpu.VMEM((query_rows, width), bf16),
            pltpu.VMEM((key_rows, kv_width), bf16),
            pltpu.VMEM((key_rows, kv_width), bf16),
            pltpu.VMEM(segment_rows.shape, jnp.int32),
        ]

    scratch = [
        pltpu.VMEM((groups, stack, 4 * WINDOW), f32),
        pltpu.VMEM((groups, stack, 4 * WINDOW), bf16),
        pltpu.VMEM((groups, stack, LANES), f32),
    ]
    flops = 16 * WINDOW * WINDOW * width
    later, tail = call(
        later_body,
        [((tokens - WINDOW, width), bf16), ((WINDOW, 2 * kv_width), bf16)],
        inputs,
        [HBM] * 5,
        local(tokens - WINDOW, tokens) + scratch,
        flops * (tokens // WINDOW - 1),
    )
    peers = lax.axis_size("seq")
    tail = lax.ppermute(tail, "seq", [(i, (i + 1) % peers) for i in range(peers)])
    columns = tokens // (2 * shard_rows)
    out_width = out_weight.shape[1]
    side = ((columns, shard_rows, out_width), bf16)
    return call(
        first_body,
        [side, side],
        inputs + [tail, later, out_weight],
        [HBM] * 5 + [VMEM] * 3,
        local(WINDOW, WINDOW) + [pltpu.VMEM((tokens, width), bf16)] + scratch,
        flops + 2 * tokens * width * out_width,
        24 << 20,
    )


def chip_body(kept_ref, taken_ref, residual_ref, hidden_ref, *away_refs):
    columns = kept_ref.shape[0]
    column = lax.axis_index("head") // 2
    total = kept_ref[column].astype(jnp.float32) + taken_ref[column].astype(jnp.float32)
    hidden_ref[...] = residual_ref[...].astype(jnp.float32) + total
    for step, away_ref in enumerate(away_refs):
        target = lax.rem(column + step + 1, columns)
        total = kept_ref[target].astype(jnp.float32) + taken_ref[target].astype(jnp.float32)
        away_ref[...] = total.astype(away_ref.dtype)


def norm_body(count, experts, partial_ref, gain_ref, ids_ref, route_ref, *refs):
    arrived = refs[:count]
    hidden_ref, packed_ref = refs[count:]
    hidden = partial_ref[...]
    for ref in arrived:
        hidden = hidden + ref[...].astype(jnp.float32)
    hidden_ref[...] = hidden
    width = hidden.shape[1]
    variance = jnp.mean(hidden * hidden, -1, keepdims=True)
    normed = hidden * lax.rsqrt(variance + 1e-05) * gain_ref[...]
    packed_ref[:, :width] = normed.astype(packed_ref.dtype)
    lane = lax.broadcasted_iota(jnp.int32, (hidden.shape[0], LANES), 1)
    name = lax.rem(lane, experts)
    dense = jnp.zeros((hidden.shape[0], LANES), jnp.float32)
    for choice in range(ids_ref.shape[1]):
        ids = ids_ref[:, choice : choice + 1]
        dense = dense + jnp.where(ids == name, route_ref[:, choice : choice + 1], 0.0)
    high = dense.astype(jnp.bfloat16)
    rest = dense - high.astype(jnp.float32)
    middle = rest.astype(jnp.bfloat16)
    low = (rest - middle.astype(jnp.float32)).astype(jnp.bfloat16)
    third = lane // experts
    coded = jnp.where(
        third == 0,
        high.astype(jnp.float32),
        jnp.where(
            third == 1,
            middle.astype(jnp.float32),
            jnp.where(third == 2, low.astype(jnp.float32), 0.0),
        ),
    )
    packed_ref[:, width:] = coded.astype(packed_ref.dtype)


def ffn_body(experts, gate_ref, up_ref, down_ref, *refs):
    ins, (keep_ref, give_ref, rows_ref, act_ref) = refs[:-4], refs[-4:]
    width, hidden = gate_ref.shape[1], gate_ref.shape[2]
    half = keep_ref.shape[0]
    expert = (lax.axis_index("seq") * lax.axis_size("head") + lax.axis_index("head")) // 2
    scales = []
    start = 0
    for ref in ins:
        count = ref.shape[0]
        rows_ref[start : start + count, :] = ref[:, :width]
        coded = ref[:, width:].astype(jnp.float32)
        lane = lax.broadcasted_iota(jnp.int32, coded.shape, 1)
        mine = (lane == expert) | (lane == expert + experts) | (lane == expert + 2 * experts)
        scales.append(jnp.sum(jnp.where(mine, coded, 0.0), -1, keepdims=True))
        start += count
    scale = jnp.concatenate(scales, 0)
    tile = 256 if hidden % 256 == 0 else hidden
    for low in range(0, hidden, tile):
        cols = slice(low, low + tile)
        gate_val = jnp.minimum(
            jnp.dot(rows_ref[...], gate_ref[0, :, cols], preferred_element_type=jnp.float32), 7.0
        )
        up_val = jnp.clip(
            jnp.dot(rows_ref[...], up_ref[0, :, cols], preferred_element_type=jnp.float32),
            -7.0,
            7.0,
        )
        act_ref[:, cols] = ((up_val + 1.0) * gate_val * jax.nn.sigmoid(1.702 * gate_val)).astype(
            act_ref.dtype
        )
    tile = 512 if width % 512 == 0 else width
    for low in range(0, width, tile):
        cols = slice(low, low + tile)
        value = jnp.dot(act_ref[...], down_ref[0, :, cols], preferred_element_type=jnp.float32)
        value = (value * scale).astype(keep_ref.dtype)
        keep_ref[:, cols] = value[:half]
        give_ref[:, cols] = value[half:]


def ring_layer(
    query_states,
    key_states,
    value_states,
    sink_logits,
    segment_ids,
    residual,
    out_weight,
    norm_gain,
    expert_ids,
    route_weights,
    gate_proj,
    up_proj,
    down_proj,
):
    shard_rows, width = residual.shape
    hidden_units = gate_proj.shape[2]
    seq, head = lax.axis_size("seq"), lax.axis_size("head")
    columns = head // 2
    chips = seq * columns

    order = [
        (col, row if col % 2 == 0 else seq - 1 - row) for col in range(columns) for row in range(seq)
    ]

    def device(place, which):
        col, row = order[place % chips]
        return row * head + col * 2 + which

    onward = [(device(p, c), device(p + 1, c)) for p in range(chips) for c in range(2)]
    back = [(b, a) for a, b in onward]

    def ring(pair):
        on = lax.ppermute(pair[0], ("seq", "head"), onward)
        off = lax.ppermute(pair[1], ("seq", "head"), back)
        return on, off

    def swap(value):
        return partner(value, "head", 0)

    bf16, f32 = jnp.bfloat16, jnp.float32
    out_weight, residual = loaded([out_weight, residual])
    kept, given = projected_heads(
        query_states, key_states, value_states, sink_logits, segment_ids, out_weight, shard_rows
    )
    rows = (shard_rows, width)
    hidden_state, *away = call(
        chip_body,
        [(rows, f32)] + [(rows, bf16)] * (columns - 1),
        [kept, swap(given), residual],
        [VMEM] * 3,
    )
    arrived = []
    for step, value in enumerate(away):
        pairs = [(i, (i + 2 * (step + 1)) % head) for i in range(head)]
        arrived.append(lax.ppermute(value, "head", pairs))
    gate_proj, up_proj, down_proj = loaded([gate_proj, up_proj, down_proj])
    packed = (shard_rows, width + LANES)
    hidden_state, mine = call(
        functools.partial(norm_body, len(arrived), chips),
        [(rows, f32), (packed, bf16)],
        [hidden_state, norm_gain.reshape(1, -1), expert_ids, route_weights] + arrived,
        [VMEM] * (4 + len(arrived)),
    )

    def terms(blocks):
        count = 2 * sum(block.shape[0] for block in blocks)
        others = []
        for block in blocks:
            others.append(swap(block))
        out = ((count // 2, width), bf16)
        keep, give = call(
            functools.partial(ffn_body, chips),
            [out, out],
            [gate_proj, up_proj, down_proj] + blocks + others,
            [VMEM] * (3 + 2 * len(blocks)),
            [pltpu.VMEM((count, width), bf16), pltpu.VMEM((count, hidden_units), bf16)],
            6 * count * width * hidden_units,
            24 << 20,
        )
        taken = swap(give)
        return keep.astype(jnp.float32) + taken.astype(jnp.float32)

    half = shard_rows // 2
    own_term = terms([mine])
    sums = []
    travelling = (mine, mine)
    for _ in range(1, chips // 2):
        travelling = ring(travelling)
        sums.append(terms(list(travelling)))
    travelling = ring((travelling[0][:half], travelling[1][half:]))
    total = terms(list(travelling)).astype(jnp.bfloat16)
    passing = ring((total[:half], total[half:]))
    for total in reversed(sums):
        on, off = (value.astype(jnp.float32) for value in passing)
        if on.shape[0] < shard_rows:
            on = jnp.pad(on, ((0, half), (0, 0)))
            off = jnp.pad(off, ((half, 0), (0, 0)))
        on = (total[shard_rows:] + on).astype(jnp.bfloat16)
        off = (total[:shard_rows] + off).astype(jnp.bfloat16)
        passing = ring((on, off))
    on, off = (value.astype(jnp.float32) for value in passing)
    if on.shape[0] < shard_rows:
        on = jnp.concatenate([on, off], 0)
        off = 0.0
    return (hidden_state + (on + off + own_term)).astype(jnp.bfloat16)


def per_device(query_states, key_states, value_states, sink_logits, segment_ids, *rest):
    residual, _, _, expert_ids = rest[:4]
    seq, head, pair = lax.axis_size("seq"), lax.axis_size("head"), lax.axis_size("pair")
    experts = seq * head // 2
    dense_pays = 2 * expert_ids.shape[1] >= experts
    ring_fits = pair == 1 and head % 2 == 0 and experts % 2 == 0 and 3 * experts <= LANES
    shard_rows = residual.shape[0]
    tokens, width = query_states.shape
    kv_width = key_states.shape[1]
    rows_fit = shard_rows % 32 == 0 and tokens % WINDOW == 0 and WINDOW % min(shard_rows, WINDOW) == 0
    heads_fit = kv_width % LANES == 0 and width % (2 * kv_width) == 0
    if dense_pays and ring_fits and rows_fit and heads_fit:
        return ring_layer(query_states, key_states, value_states, sink_logits, segment_ids, *rest)
    attended = attention(query_states, key_states, value_states, sink_logits, segment_ids)
    return exchanged_layer(attended, *rest)


def solution(mesh):
    in_specs = (
        P(("group", "seq"), ("head", "pair")),
        P(("group", "seq"), "head"),
        P(("group", "seq"), "head"),
        P(("head", "pair")),
        P("group"),
        P(("group", "seq", "head", "pair"), None),
        P(("head", "pair"), None),
        P(),
        P(("group", "seq", "head", "pair"), None),
        P(("group", "seq", "head", "pair"), None),
        P(("seq", "head"), None, "pair"),
        P(("seq", "head"), None, "pair"),
        P(("seq", "head"), "pair", None),
    )
    out_specs = P(("group", "seq", "head", "pair"), None)
    return jax.shard_map(
        per_device, mesh=mesh, in_specs=in_specs, out_specs=out_specs, check_vma=False
    )
```

```python
import functools

import jax
import jax.numpy as jnp
from jax import lax
from jax.experimental import pallas as pl
from jax.experimental.pallas import tpu as pltpu
from jax.sharding import PartitionSpec as P


HEADS = 64
KV_HEADS = 8
HEAD_DIM = 64
WINDOW = 128
LANES = 128


def passed_along(value, axis, by):
    peers = lax.axis_size(axis)
    pairs = [(i, i + by) for i in range(peers) if 0 <= i + by < peers]
    return lax.ppermute(value, axis, pairs)


def partner(value, axis, distance):
    return lax.ppermute(value, axis, [(i, i ^ 1 << distance) for i in range(lax.axis_size(axis))])


def round_keep(values):
    return lax.optimization_barrier(values.astype(jnp.bfloat16)).astype(jnp.float32)


def window_attention(
    query_block, key_block, value_block, query_pos, key_pos, query_seg, key_seg, sink_logits
):
    scores = jnp.einsum(
        "qhd,khd->hqk", query_block, key_block, preferred_element_type=jnp.float32
    ) * HEAD_DIM ** (-0.5)
    visible = (key_pos[None, :] <= query_pos[:, None]) & (
        query_pos[:, None] - key_pos[None, :] < WINDOW
    )
    visible = visible & (key_pos[None, :] >= 0) & (key_seg[None, :] == query_seg[:, None])
    masked = jnp.where(visible[None], scores, -1e30)
    row_max = jnp.maximum(jnp.max(masked, -1), sink_logits[:, None])
    weights_exp = jnp.exp(masked - row_max[..., None])
    denominator = jnp.sum(weights_exp, -1) + jnp.exp(sink_logits[:, None] - row_max)
    probs = (weights_exp / denominator[..., None]).astype(jnp.bfloat16)
    attended = jnp.einsum("hqk,khd->qhd", probs, value_block, preferred_element_type=jnp.float32)
    return attended.astype(jnp.bfloat16)


def attention(query_states, key_states, value_states, sink_logits, segment_ids):
    tok_rows = query_states.shape[0]
    local_heads = query_states.shape[1] // HEAD_DIM
    local_groups = key_states.shape[1] // HEAD_DIM
    group_size = HEADS // KV_HEADS
    tail_keys, tail_values = passed_along(
        (key_states[tok_rows - WINDOW :], value_states[tok_rows - WINDOW :]), "seq", 1
    )
    ext_keys = jnp.concatenate([tail_keys, key_states], 0).reshape(
        tok_rows + WINDOW, local_groups, HEAD_DIM
    )
    ext_values = jnp.concatenate([tail_values, value_states], 0).reshape(
        tok_rows + WINDOW, local_groups, HEAD_DIM
    )
    kv_owner = (
        lax.axis_index("pair") * local_heads + jnp.arange(local_heads, dtype=jnp.int32)
    ) // group_size
    head_select = (kv_owner[:, None] == jnp.arange(local_groups, dtype=jnp.int32)[None, :]).astype(
        jnp.bfloat16
    )
    keys_per_head = jnp.einsum(
        "kcd,hc->khd", ext_keys, head_select, preferred_element_type=jnp.float32
    ).astype(jnp.bfloat16)
    values_per_head = jnp.einsum(
        "kcd,hc->khd", ext_values, head_select, preferred_element_type=jnp.float32
    ).astype(jnp.bfloat16)
    query_heads = query_states.reshape(tok_rows, local_heads, HEAD_DIM)
    seq_start = lax.axis_index("seq") * tok_rows
    seg_padded = jnp.concatenate([jnp.full((WINDOW,), -1, jnp.int32), segment_ids], 0)
    block_rows = min(512, tok_rows)

    def attend(block_index):
        first_row = block_index * block_rows
        query_pos = seq_start + first_row + jnp.arange(block_rows, dtype=jnp.int32)
        key_pos = seq_start + first_row - WINDOW + jnp.arange(block_rows + WINDOW, dtype=jnp.int32)
        query_seg = lax.dynamic_slice_in_dim(segment_ids, seq_start + first_row, block_rows, 0)
        key_seg = lax.dynamic_slice_in_dim(
            seg_padded, seq_start + first_row, block_rows + WINDOW, 0
        )
        return window_attention(
            query_heads,
            keys_per_head,
            values_per_head,
            query_pos,
            key_pos,
            query_seg,
            key_seg,
            sink_logits,
        )

    attended = lax.map(attend, jnp.arange(tok_rows // block_rows, dtype=jnp.int32))
    return attended.reshape(tok_rows, local_heads * HEAD_DIM)


def rms_normed(hidden_state, norm_gain):
    variance = jnp.mean(hidden_state * hidden_state, -1, keepdims=True)
    return (hidden_state * lax.rsqrt(variance + 1e-05) * norm_gain).astype(jnp.bfloat16)


def exchanged_layer(
    attended,
    residual,
    out_weight,
    norm_gain,
    expert_ids,
    route_weights,
    gate_proj,
    up_proj,
    down_proj,
):
    shard_rows = residual.shape[0]
    width = residual.shape[1]
    projected = lax.psum_scatter(
        round_keep(jnp.dot(attended, out_weight, preferred_element_type=jnp.float32)).astype(
            jnp.bfloat16
        ),
        ("head", "pair"),
        scatter_dimension=0,
        tiled=True,
    ).astype(jnp.float32)
    hidden_state = residual.astype(jnp.float32) + projected
    normed = rms_normed(hidden_state, norm_gain)
    top_count = expert_ids.shape[1]
    experts = lax.axis_size("seq") * lax.axis_size("head") // 2
    capacity = min(shard_rows, max(2, 3 * shard_rows * top_count // (2 * experts)))
    flat_ids = expert_ids.reshape(-1)
    onehot = (flat_ids[:, None] == jnp.arange(experts, dtype=jnp.int32)[None, :]).astype(jnp.int32)
    before = jnp.cumsum(onehot, axis=0, dtype=jnp.int32) - onehot
    slot_rank = jnp.sum(before * onehot, -1)
    slot_index = flat_ids * capacity + slot_rank
    dispatch_mat = (
        slot_index[None, :] == jnp.arange(experts * capacity, dtype=jnp.int32)[:, None]
    ).astype(jnp.bfloat16)
    repeated = jnp.repeat(normed, top_count, axis=0)
    outgoing = jnp.dot(dispatch_mat, repeated, preferred_element_type=jnp.float32).astype(
        jnp.bfloat16
    )
    outgoing = outgoing.reshape(experts, capacity, width)
    half_idx = lax.axis_index("head") % 2
    half_width = width // 2
    split_rows = outgoing.reshape(experts, capacity, 2, half_width).transpose(0, 2, 1, 3)
    split_rows = split_rows.reshape(2 * experts, capacity, half_width)
    own_half = lax.all_to_all(split_rows, ("seq", "head"), split_axis=0, concat_axis=0, tiled=True)
    other_half = partner(own_half, "head", 0)
    arrived = jnp.where(
        half_idx == 0,
        jnp.concatenate([own_half, other_half], -1),
        jnp.concatenate([other_half, own_half], -1),
    )
    piece_rows = lax.all_gather(arrived, "pair", axis=0, tiled=True)
    flat_rows = piece_rows.reshape(-1, width)
    gate_val = jnp.minimum(
        jnp.dot(flat_rows, gate_proj[0], preferred_element_type=jnp.float32), 7.0
    )
    up_val = jnp.clip(
        jnp.dot(flat_rows, up_proj[0], preferred_element_type=jnp.float32), -7.0, 7.0
    )
    activated = ((up_val + 1.0) * gate_val * jax.nn.sigmoid(1.702 * gate_val)).astype(jnp.bfloat16)
    partial_value = round_keep(jnp.dot(activated, down_proj[0], preferred_element_type=jnp.float32))
    quarter_terms = partial_value.reshape(piece_rows.shape)
    pair_sums = lax.psum_scatter(
        quarter_terms.astype(jnp.bfloat16), "pair", scatter_dimension=0, tiled=True
    ).astype(jnp.float32)
    kept_half = lax.dynamic_slice_in_dim(pair_sums, half_idx * half_width, half_width, 2)
    given_half = lax.dynamic_slice_in_dim(pair_sums, (1 - half_idx) * half_width, half_width, 2)
    partner_half = partner(given_half.astype(jnp.bfloat16), "head", 0).astype(given_half.dtype)
    merged = kept_half + partner_half
    returned = lax.all_to_all(
        merged.astype(jnp.bfloat16), ("seq", "head"), split_axis=0, concat_axis=0, tiled=True
    ).astype(merged.dtype)
    expert_out = (
        returned.reshape(experts, 2, capacity, half_width)
        .transpose(0, 2, 1, 3)
        .reshape(experts, capacity, width)
    )
    slot_table = slot_index.reshape(shard_rows, top_count)
    columns_all = jnp.arange(experts * capacity, dtype=jnp.int32)
    combine_mat = jnp.sum(
        jnp.where(
            slot_table[:, :, None] == columns_all[None, None, :], route_weights[:, :, None], 0.0
        ),
        axis=1,
    )
    mixture = jnp.dot(
        combine_mat, expert_out.reshape(experts * capacity, width), precision=lax.Precision.HIGHEST
    )
    return (hidden_state + mixture).astype(jnp.bfloat16)


def attend_block(
    query, window_keys, window_values, bias, sink_ref, score_ref, prob_ref, inverse_ref, store
):
    rows = query.shape[0]
    span = window_keys.shape[0]
    groups = window_keys.shape[1] // HEAD_DIM
    tiles = query.shape[1] // LANES // groups
    lane = lax.broadcasted_iota(jnp.int32, (span, LANES), 1)
    out_lane = lax.broadcasted_iota(jnp.int32, (rows, LANES), 1)

    def both_sides(values, group):
        tile = values[:, group // 2 * LANES : (group // 2 + 1) * LANES]
        here = jnp.where(lane // HEAD_DIM == group % 2, tile, 0.0)
        there = pltpu.roll(here, HEAD_DIM, 1)
        sides = [here, there] if group % 2 == 0 else [there, here]
        return jnp.concatenate(sides, 0).astype(jnp.bfloat16)

    for group in range(groups):
        keys = both_sides(window_keys.astype(jnp.float32) * HEAD_DIM**-0.5, group)
        first = group * tiles
        stacked = jnp.concatenate(
            [query[:, (first + t) * LANES : (first + t + 1) * LANES] for t in range(tiles)], 0
        )
        score_ref[group] = lax.dot_general(
            stacked, keys, (((1,), (1,)), ((), ())), preferred_element_type=jnp.float32
        )
    for group in range(groups):
        first = group * tiles
        for t in range(tiles):
            at = slice(t * rows, (t + 1) * rows)
            inverses = []
            for side in range(2):
                cols = slice(side * span, (side + 1) * span)
                sink = sink_ref[2 * (first + t) + side]
                masked = score_ref[group, at, cols] + bias
                top = jnp.maximum(jnp.max(masked, -1, keepdims=True), sink)
                weights = jnp.exp(masked - top)
                total = jnp.sum(weights, -1, keepdims=True) + jnp.exp(sink - top)
                prob_ref[group, at, cols] = weights.astype(jnp.bfloat16)
                inverses.append(1.0 / total)
            inverse_ref[group, at, :] = jnp.where(out_lane < HEAD_DIM, inverses[0], inverses[1])
    for group in range(groups):
        first = group * tiles
        values = both_sides(window_values.astype(jnp.float32), group)
        out = jnp.dot(prob_ref[group], values, preferred_element_type=jnp.float32)
        out = (out * inverse_ref[group]).astype(jnp.bfloat16)
        for t in range(tiles):
            store(first + t, out[t * rows : (t + 1) * rows])


def visible_bias(segment_ref, before, here, starts):
    row = segment_ref[pl.ds(here, 1), :]
    prior = jnp.where(starts, -1, segment_ref[pl.ds(before, 1), :])
    block = (WINDOW, WINDOW)
    own = jnp.transpose(jnp.broadcast_to(row, block).astype(jnp.float32))
    query_at = lax.broadcasted_iota(jnp.int32, block, 0)
    key_at = lax.broadcasted_iota(jnp.int32, block, 1)
    earlier = (key_at > query_at) & (own == prior.astype(jnp.float32))
    later = (key_at <= query_at) & (own == row.astype(jnp.float32))
    seen = jnp.concatenate([earlier, later], 1)
    return jnp.where(seen, 0.0, -1e30)


def fetch(sources, targets, sems):
    copies = [
        pltpu.make_async_copy(source, target, sems.at[i])
        for i, (source, target) in enumerate(zip(sources, targets))
    ]
    for copy in copies:
        copy.start()
    for copy in copies:
        copy.wait()


def load_body(*refs):
    count = len(refs) // 2
    fetch(refs[:count], refs[count:-1], refs[-1])


def later_body(
    sink_any,
    query_any,
    key_any,
    value_any,
    segment_any,
    out_ref,
    tail_ref,
    sems,
    sink_ref,
    query_ref,
    key_ref,
    value_ref,
    segment_ref,
    *scratch,
):
    tokens = key_ref.shape[0]
    blocks = tokens // WINDOW
    kv_width = key_ref.shape[1]
    fetch(
        [sink_any, query_any.at[WINDOW:, :], key_any, value_any, segment_any],
        [sink_ref, query_ref, key_ref, value_ref, segment_ref],
        sems,
    )
    tail_ref[:, :kv_width] = key_ref[tokens - WINDOW :, :]
    tail_ref[:, kv_width:] = value_ref[tokens - WINDOW :, :]
    for block in range(1, blocks):
        here = lax.axis_index("seq") * blocks + block
        bias = visible_bias(segment_ref, here - 1, here, False)
        rows = slice((block - 1) * WINDOW, block * WINDOW)
        window = slice((block - 1) * WINDOW, (block + 1) * WINDOW)

        def store(tile, value, rows=rows):
            out_ref[rows, tile * LANES : (tile + 1) * LANES] = value

        attend_block(
            query_ref[rows, :],
            key_ref[window, :],
            value_ref[window, :],
            bias,
            sink_ref,
            *scratch,
            store,
        )


def first_body(
    sink_any,
    query_any,
    key_any,
    value_any,
    segment_any,
    tail_ref,
    later_ref,
    weight_ref,
    kept_ref,
    given_ref,
    sems,
    sink_ref,
    query_ref,
    key_ref,
    value_ref,
    segment_ref,
    sorted_ref,
    *scratch,
):
    tokens = later_ref.shape[0] + WINDOW
    half = tokens // 2
    shard_rows = kept_ref.shape[1]
    piece = min(shard_rows, WINDOW)
    core = lax.axis_index("head") % 2
    here = lax.axis_index("seq") * (tokens // WINDOW)
    kv_width = key_ref.shape[1]
    fetch(
        [
            sink_any,
            query_any.at[:WINDOW, :],
            key_any.at[:WINDOW, :],
            value_any.at[:WINDOW, :],
            segment_any,
        ],
        [sink_ref, query_ref, key_ref, value_ref, segment_ref],
        sems,
    )
    bias = visible_bias(segment_ref, jnp.maximum(here - 1, 0), here, here == 0)

    def goal(row):
        owner = row // shard_rows
        side = jnp.where(core == owner % 2, 0, half)
        return pl.multiple_of(side + owner // 2 * shard_rows + row % shard_rows, piece)

    for row in range(WINDOW, tokens, piece):
        sorted_ref[pl.ds(goal(row), piece), :] = later_ref[row - WINDOW : row - WINDOW + piece, :]

    def store(tile, value):
        for row in range(0, WINDOW, piece):
            sorted_ref[pl.ds(goal(row), piece), tile * LANES : (tile + 1) * LANES] = value[
                row : row + piece
            ]

    attend_block(
        query_ref[...],
        jnp.concatenate([tail_ref[:, :kv_width], key_ref[...]], 0),
        jnp.concatenate([tail_ref[:, kv_width:], value_ref[...]], 0),
        bias,
        sink_ref,
        *scratch,
        store,
    )
    width = weight_ref.shape[1]
    columns = kept_ref.shape[0]
    tile = 512 if width % 512 == 0 else width
    for low in range(0, width, tile):
        cols = slice(low, low + tile)
        value = jnp.dot(
            sorted_ref[...], weight_ref[:, cols], preferred_element_type=jnp.float32
        ).astype(jnp.bfloat16)
        for column in range(columns):
            at = column * shard_rows
            kept_ref[column, :, cols] = value[at : at + shard_rows]
            given_ref[column, :, cols] = value[half + at : half + at + shard_rows]


VMEM = pl.BlockSpec(memory_space=pltpu.VMEM)
HBM = pl.BlockSpec(memory_space=pltpu.HBM)


def call(body, outs, args, specs, scratch=(), flops=0, limit=16 << 20):
    moved = sum(a.size * a.dtype.itemsize for a in args)
    return pl.pallas_call(
        body,
        out_shape=[pltpu.VMEM(shape, dtype) for shape, dtype in outs],
        in_specs=specs,
        out_specs=[VMEM] * len(outs),
        scratch_shapes=list(scratch),
        compiler_params=pltpu.CompilerParams(vmem_limit_bytes=limit),
        cost_estimate=pl.CostEstimate(flops=flops, bytes_accessed=moved, transcendentals=0),
    )(*args)


def loaded(args, limit):
    return call(
        load_body,
        [(a.shape, a.dtype) for a in args],
        args,
        [HBM] * len(args),
        [pltpu.SemaphoreType.DMA((len(args),))],
        limit=limit << 20,
    )


def projected_heads(
    query_states, key_states, value_states, sink_logits, segment_ids, out_weight, shard_rows
):
    tokens, width = query_states.shape
    kv_width = key_states.shape[1]
    groups = kv_width // HEAD_DIM
    stack = width // LANES // groups * WINDOW
    segment_rows = segment_ids.reshape(-1, WINDOW)
    inputs = [sink_logits, query_states, key_states, value_states, segment_rows]
    bf16, f32 = jnp.bfloat16, jnp.float32

    def local(query_rows, key_rows):
        return [
            pltpu.SemaphoreType.DMA((len(inputs),)),
            pltpu.SMEM(sink_logits.shape, f32),
            pltpu.VMEM((query_rows, width), bf16),
            pltpu.VMEM((key_rows, kv_width), bf16),
            pltpu.VMEM((key_rows, kv_width), bf16),
            pltpu.VMEM(segment_rows.shape, jnp.int32),
        ]

    scratch = [
        pltpu.VMEM((groups, stack, 4 * WINDOW), f32),
        pltpu.VMEM((groups, stack, 4 * WINDOW), bf16),
        pltpu.VMEM((groups, stack, LANES), f32),
    ]
    flops = 16 * WINDOW * WINDOW * width
    later, tail = call(
        later_body,
        [((tokens - WINDOW, width), bf16), ((WINDOW, 2 * kv_width), bf16)],
        inputs,
        [HBM] * 5,
        local(tokens - WINDOW, tokens) + scratch,
        flops * (tokens // WINDOW - 1),
        60 << 20,
    )
    peers = lax.axis_size("seq")
    tail = lax.ppermute(tail, "seq", [(i, (i + 1) % peers) for i in range(peers)])
    columns = tokens // (2 * shard_rows)
    out_width = out_weight.shape[1]
    side = ((columns, shard_rows, out_width), bf16)
    return call(
        first_body,
        [side, side],
        inputs + [tail, later, out_weight],
        [HBM] * 5 + [VMEM] * 3,
        local(WINDOW, WINDOW) + [pltpu.VMEM((tokens, width), bf16)] + scratch,
        flops + 2 * tokens * width * out_width,
        24 << 20,
    )


def chip_body(kept_ref, taken_ref, residual_ref, hidden_ref, *away_refs):
    columns = kept_ref.shape[0]
    column = lax.axis_index("head") // 2
    total = kept_ref[column].astype(jnp.float32) + taken_ref[column].astype(jnp.float32)
    hidden_ref[...] = residual_ref[...].astype(jnp.float32) + total
    for step, away_ref in enumerate(away_refs):
        target = lax.rem(column + step + 1, columns)
        total = kept_ref[target].astype(jnp.float32) + taken_ref[target].astype(jnp.float32)
        away_ref[...] = total.astype(away_ref.dtype)


def norm_body(count, experts, partial_ref, gain_ref, ids_ref, route_ref, *refs):
    arrived = refs[:count]
    hidden_ref, packed_ref = refs[count:]
    hidden = partial_ref[...]
    for ref in arrived:
        hidden = hidden + ref[...].astype(jnp.float32)
    hidden_ref[...] = hidden
    width = hidden.shape[1]
    variance = jnp.mean(hidden * hidden, -1, keepdims=True)
    normed = hidden * lax.rsqrt(variance + 1e-05) * gain_ref[...]
    packed_ref[:, :width] = normed.astype(packed_ref.dtype)
    lane = lax.broadcasted_iota(jnp.int32, (hidden.shape[0], LANES), 1)
    name = lax.rem(lane, experts)
    dense = jnp.zeros((hidden.shape[0], LANES), jnp.float32)
    for choice in range(ids_ref.shape[1]):
        ids = ids_ref[:, choice : choice + 1]
        dense = dense + jnp.where(ids == name, route_ref[:, choice : choice + 1], 0.0)
    high = dense.astype(jnp.bfloat16)
    rest = dense - high.astype(jnp.float32)
    middle = rest.astype(jnp.bfloat16)
    low = (rest - middle.astype(jnp.float32)).astype(jnp.bfloat16)
    third = lane // experts
    coded = jnp.where(
        third == 0,
        high.astype(jnp.float32),
        jnp.where(
            third == 1,
            middle.astype(jnp.float32),
            jnp.where(third == 2, low.astype(jnp.float32), 0.0),
        ),
    )
    packed_ref[:, width:] = coded.astype(packed_ref.dtype)


def ffn_body(experts, gate_ref, up_ref, down_ref, *refs):
    ins, (keep_ref, give_ref, rows_ref, act_ref) = refs[:-4], refs[-4:]
    width, hidden = gate_ref.shape[1], gate_ref.shape[2]
    half = keep_ref.shape[0]
    expert = (lax.axis_index("seq") * lax.axis_size("head") + lax.axis_index("head")) // 2
    scales = []
    start = 0
    for ref in ins:
        count = ref.shape[0]
        rows_ref[start : start + count, :] = ref[:, :width]
        coded = ref[:, width:].astype(jnp.float32)
        lane = lax.broadcasted_iota(jnp.int32, coded.shape, 1)
        mine = (lane == expert) | (lane == expert + experts) | (lane == expert + 2 * experts)
        scales.append(jnp.sum(jnp.where(mine, coded, 0.0), -1, keepdims=True))
        start += count
    scale = jnp.concatenate(scales, 0)
    tile = 256 if hidden % 256 == 0 else hidden
    for low in range(0, hidden, tile):
        cols = slice(low, low + tile)
        gate_val = jnp.minimum(
            jnp.dot(rows_ref[...], gate_ref[0, :, cols], preferred_element_type=jnp.float32), 7.0
        )
        up_val = jnp.clip(
            jnp.dot(rows_ref[...], up_ref[0, :, cols], preferred_element_type=jnp.float32),
            -7.0,
            7.0,
        )
        act_ref[:, cols] = ((up_val + 1.0) * gate_val * jax.nn.sigmoid(1.702 * gate_val)).astype(
            act_ref.dtype
        )
    tile = 512 if width % 512 == 0 else width
    for low in range(0, width, tile):
        cols = slice(low, low + tile)
        value = jnp.dot(act_ref[...], down_ref[0, :, cols], preferred_element_type=jnp.float32)
        value = (value * scale).astype(keep_ref.dtype)
        keep_ref[:, cols] = value[:half]
        give_ref[:, cols] = value[half:]


def ring_layer(
    query_states,
    key_states,
    value_states,
    sink_logits,
    segment_ids,
    residual,
    out_weight,
    norm_gain,
    expert_ids,
    route_weights,
    gate_proj,
    up_proj,
    down_proj,
):
    shard_rows, width = residual.shape
    hidden_units = gate_proj.shape[2]
    seq, head = lax.axis_size("seq"), lax.axis_size("head")
    columns = head // 2
    chips = seq * columns

    order = [
        (col, row if col % 2 == 0 else seq - 1 - row) for col in range(columns) for row in range(seq)
    ]

    def device(place, which):
        col, row = order[place % chips]
        return row * head + col * 2 + which

    onward = [(device(p, c), device(p + 1, c)) for p in range(chips) for c in range(2)]
    back = [(b, a) for a, b in onward]

    def ring(pair):
        on = lax.ppermute(pair[0], ("seq", "head"), onward)
        off = lax.ppermute(pair[1], ("seq", "head"), back)
        return on, off

    def swap(value):
        return partner(value, "head", 0)

    bf16, f32 = jnp.bfloat16, jnp.float32
    out_weight, residual = loaded([out_weight, residual], 58)
    kept, given = projected_heads(
        query_states, key_states, value_states, sink_logits, segment_ids, out_weight, shard_rows
    )
    rows = (shard_rows, width)
    hidden_state, *away = call(
        chip_body,
        [(rows, f32)] + [(rows, bf16)] * (columns - 1),
        [kept, swap(given), residual],
        [VMEM] * 3,
    )
    arrived = []
    for step, value in enumerate(away):
        pairs = [(i, (i + 2 * (step + 1)) % head) for i in range(head)]
        arrived.append(lax.ppermute(value, "head", pairs))
    gate_proj, up_proj, down_proj = loaded([gate_proj, up_proj, down_proj], 54)
    packed = (shard_rows, width + LANES)
    hidden_state, mine = call(
        functools.partial(norm_body, len(arrived), chips),
        [(rows, f32), (packed, bf16)],
        [hidden_state, norm_gain.reshape(1, -1), expert_ids, route_weights] + arrived,
        [VMEM] * (4 + len(arrived)),
    )

    def terms(blocks):
        count = 2 * sum(block.shape[0] for block in blocks)
        others = []
        for block in blocks:
            others.append(swap(block))
        out = ((count // 2, width), bf16)
        keep, give = call(
            functools.partial(ffn_body, chips),
            [out, out],
            [gate_proj, up_proj, down_proj] + blocks + others,
            [VMEM] * (3 + 2 * len(blocks)),
            [pltpu.VMEM((count, width), bf16), pltpu.VMEM((count, hidden_units), bf16)],
            6 * count * width * hidden_units,
            24 << 20,
        )
        taken = swap(give)
        return keep.astype(jnp.float32) + taken.astype(jnp.float32)

    half = shard_rows // 2
    own_term = terms([mine])
    sums = []
    travelling = (mine, mine)
    for _ in range(1, chips // 2):
        travelling = ring(travelling)
        sums.append(terms(list(travelling)))
    travelling = ring((travelling[0][:half], travelling[1][half:]))
    total = terms(list(travelling)).astype(bf16)
    across = [(device(p, c), device(p + chips // 2, c)) for p in range(chips) for c in range(2)]
    mixture = own_term + lax.ppermute(total, ("seq", "head"), across).astype(f32)
    passing = None
    for step in range(chips // 2 - 1, 0, -1):
        on, off = sums[step - 1][shard_rows:], sums[step - 1][:shard_rows]
        if passing is not None:
            on, off = on + passing[0].astype(f32), off + passing[1].astype(f32)
        passing = ring((on.astype(bf16), off.astype(bf16)))
    if passing is not None:
        mixture = mixture + (passing[0].astype(f32) + passing[1].astype(f32))
    return (hidden_state + mixture).astype(bf16)


def per_device(query_states, key_states, value_states, sink_logits, segment_ids, *rest):
    residual, _, _, expert_ids = rest[:4]
    seq, head, pair = lax.axis_size("seq"), lax.axis_size("head"), lax.axis_size("pair")
    experts = seq * head // 2
    dense_pays = 2 * expert_ids.shape[1] >= experts
    ring_fits = pair == 1 and head % 2 == 0 and experts % 2 == 0 and 3 * experts <= LANES
    shard_rows = residual.shape[0]
    tokens, width = query_states.shape
    kv_width = key_states.shape[1]
    rows_fit = shard_rows % 32 == 0 and tokens % WINDOW == 0 and WINDOW % min(shard_rows, WINDOW) == 0
    heads_fit = kv_width % LANES == 0 and width % (2 * kv_width) == 0
    if dense_pays and ring_fits and rows_fit and heads_fit:
        return ring_layer(query_states, key_states, value_states, sink_logits, segment_ids, *rest)
    attended = attention(query_states, key_states, value_states, sink_logits, segment_ids)
    return exchanged_layer(attended, *rest)


def solution(mesh):
    in_specs = (
        P(("group", "seq"), ("head", "pair")),
        P(("group", "seq"), "head"),
        P(("group", "seq"), "head"),
        P(("head", "pair")),
        P("group"),
        P(("group", "seq", "head", "pair"), None),
        P(("head", "pair"), None),
        P(),
        P(("group", "seq", "head", "pair"), None),
        P(("group", "seq", "head", "pair"), None),
        P(("seq", "head"), None, "pair"),
        P(("seq", "head"), None, "pair"),
        P(("seq", "head"), "pair", None),
    )
    out_specs = P(("group", "seq", "head", "pair"), None)
    return jax.shard_map(
        per_device, mesh=mesh, in_specs=in_specs, out_specs=out_specs, check_vma=False
    )
```
